32 devices in a mesh: sims: 2 (over x), rows: 4 (over y, core), fields: 4 (over z).
Axes of the slice: x: 2, y: 2, z: 4, core: 2. Of those that a mesh axis runs over, the one named last changes fastest.
Arguments:
- sky_maps: float32 [6, 32, 16384], P('sims', 'rows', 'fields'), parts along dimension 0, may hold values from -7 to 7
- band_cuts: int32 [6], replicated, may hold values from 1 to 8191, as said below
- filters: float32 [3, 32, 16384], P(None, ('rows', 'fields')), may hold values from 0.3 to 3
- wiener: float32 [2, 32, 16384], P(None, ('rows', 'fields')), may hold values from 0.3 to 3
- response: float32 [32, 16384], P(('rows', 'fields')), may hold values from 0.5 to 2
Outputs:
- phi_curl: float32 [4, 32, 16384], P('sims', 'rows', 'fields'), parts along dimension 0
The draws below stay inside these ranges and needn't reach their ends.
There are 2 independent parts, one for each index of `sims`. The reference program is written for one: setup_inputs(seed, part) draws one part's arguments, and reference() takes and returns one part's arrays. A program takes and returns all parts, laid end to end along the dimension named above; an argument that names none is the same for every part. Nothing has to cross between parts.
Inputs may be any that keep to these rules, and one draw needn't show every extreme that they name: `band_cuts`: entries 0, 2 and 4 are the smallest multipole indices of the temperature, polarization and estimate bands and lie below 512; entries 1, 3 and 5 are the largest and are at least 4096.
All inputs are finite; a program needn't handle non-finite values.
Results may differ from the reference program's by a relative error of at most 0.00019.
Values sent between devices are 32-bit elements; how exact they have to be, the bound alone decides.
A program may use at most 128 MiB of HBM per device.

```python
import math
import jax
import jax.numpy as jnp

NC = 16384
NR = 32


def draw_sky_maps(key, part):
    rough_part = jax.random.normal(key, (3, NR, NC), jnp.float32)
    return jnp.clip(rough_part, -7.0, 7.0)


def draw_band_cuts(key, part):
    low_key = jax.random.fold_in(key, 3)
    high_key = jax.random.fold_in(key, 5)
    lowest = jax.random.randint(low_key, (3,), 1, max(2, NC // 32), dtype=jnp.int32)
    highest = jax.random.randint(high_key, (3,), NC // 4, NC // 2, dtype=jnp.int32)
    return jnp.stack([lowest, highest], axis=1).reshape(6)


def steps_of(own_key, shape, split, smallest, top_value):
    factor_of, own = 1.0, jax.random.fold_in(own_key, 6)
    for dim, parts in split:
        heights = jnp.exp(jax.random.uniform(jax.random.fold_in(own, dim), (parts,), jnp.float32, smallest / len(split), top_value / len(split)))
        factor_of = factor_of * jnp.repeat(heights, shape[dim] // parts).reshape([-1 if axis == dim else 1 for axis in range(len(shape))])
    return factor_of


def setup_inputs(seed: int = 0, part: int = 0) -> dict:
    keys = jax.random.split(jax.random.key(seed), 6)
    own_keys = jax.random.split(jax.random.fold_in(keys[5], part), 6)
    return {
        "sky_maps": draw_sky_maps(jax.random.fold_in(jax.random.fold_in(keys[5], part), 71), part),
        "band_cuts": draw_band_cuts(jax.random.fold_in(keys[5], 71), part),
        "filters": jnp.clip(jnp.exp(math.log(3.0) - 2.3025851 * jax.random.uniform(keys[2], (3, NR, NC), jnp.float32) ** steps_of(keys[2], (3, NR, NC), ((1, 16),), -0.2, 0.2)), 0.3, 3.0),
        "wiener": jnp.clip(jnp.exp(math.log(3.0) - 2.3025851 * jax.random.uniform(keys[3], (2, NR, NC), jnp.float32) ** steps_of(keys[3], (2, NR, NC), ((1, 16),), -0.2, 0.2)), 0.3, 3.0),
        "response": jnp.clip(jnp.exp(math.log(2.0) - 1.3862944 * jax.random.uniform(keys[4], (NR, NC), jnp.float32) ** steps_of(keys[4], (NR, NC), ((0, 16),), -0.2, 0.2)), 0.5, 2.0),
    }


def signed_index(length):
    indices = jnp.arange(length, dtype=jnp.int32)
    return jnp.where(indices < length // 2, indices, indices - length)


def reference(sky_maps, band_cuts, filters, wiener, response):
    row_ratio = NC // NR
    freq_rows = signed_index(NR)[:, None]
    freq_cols = signed_index(NC)[None, :]
    scaled_rows = row_ratio * freq_rows
    radius_sq = freq_cols * freq_cols + scaled_rows * scaled_rows

    def band_mask(lower_cut, upper_cut):
        inside = (radius_sq >= lower_cut * lower_cut) & (radius_sq <= upper_cut * upper_cut)
        return inside.astype(jnp.float32)

    mask_temp = band_mask(band_cuts[0], band_cuts[1])
    mask_pol = band_mask(band_cuts[2], band_cuts[3])
    mask_out = band_mask(band_cuts[4], band_cuts[5])
    radius_floor = jnp.maximum(radius_sq, 1).astype(jnp.float32)
    cos_two = (freq_cols * freq_cols - scaled_rows * scaled_rows).astype(jnp.float32) / radius_floor
    sin_two = (2 * freq_cols * scaled_rows).astype(jnp.float32) / radius_floor
    along_x = (2 * freq_cols).astype(jnp.float32) / NC
    along_y = (2 * freq_rows).astype(jnp.float32) / NR
    spectra = jnp.fft.fft2(sky_maps)
    temp_modes = spectra[0]
    stokes_q = spectra[1]
    stokes_u = spectra[2]
    e_modes = -(cos_two * stokes_q + sin_two * stokes_u)
    b_modes = sin_two * stokes_q - cos_two * stokes_u
    temp_bar = mask_temp * filters[0] * temp_modes
    e_bar = mask_pol * filters[1] * e_modes
    b_bar = mask_pol * filters[2] * b_modes
    rotation = cos_two + 1j * sin_two
    raising = 1j * (along_x + 1j * along_y)
    lowering = 1j * (along_x - 1j * along_y)
    pol_wiener = -(wiener[1] * e_bar) * rotation
    leg_spectra = jnp.stack([
        temp_bar,
        raising * (wiener[0] * temp_bar),
        -(e_bar + 1j * b_bar) * rotation,
        raising * pol_wiener,
        lowering * pol_wiener,
    ])
    leg_maps = jnp.fft.ifft2(leg_spectra)
    current = leg_maps[0] * leg_maps[1] + 0.5 * (jnp.conj(leg_maps[2]) * leg_maps[3] + leg_maps[2] * jnp.conj(leg_maps[4]))
    estimate = jnp.fft.ifft2(mask_out * response * (lowering * jnp.fft.fft2(current)))
    return jnp.stack([jnp.real(estimate), jnp.imag(estimate)]).astype(jnp.float32)
```

```python
import functools
import math

import jax
import jax.numpy as jnp
import numpy as np
from jax import lax
from jax.experimental import pallas as pl
from jax.experimental.pallas import tpu as pltpu
from jax.sharding import PartitionSpec as P

NC = 16384


exact_mode = lax.Precision.HIGHEST


def split_factor(length):
    best_first = 1
    for divisor in range(1, math.isqrt(length) + 1):
        if length % divisor == 0:
            best_first = divisor
    return (best_first, length // best_first)


def phase_table(left_index, right_index, period, direction):
    product = left_index[:, None] * right_index[None, :] % period
    angles = direction * 2.0 * math.pi / period * product.astype(jnp.float32)
    return (jnp.cos(angles), jnp.sin(angles))


def complex_einsum(formula, data_pair, table_pair):
    data_real, data_imag = data_pair
    table_real, table_imag = table_pair
    real_out = jnp.einsum(formula, data_real, table_real, precision=exact_mode)
    imag_out = jnp.einsum(formula, data_real, table_imag, precision=exact_mode)
    if data_imag is not None:
        real_out = real_out - jnp.einsum(formula, data_imag, table_imag, precision=exact_mode)
        imag_out = imag_out + jnp.einsum(formula, data_imag, table_real, precision=exact_mode)
    return (real_out, imag_out)


def complex_mul(left_pair, right_pair):
    return (
        left_pair[0] * right_pair[0] - left_pair[1] * right_pair[1],
        left_pair[0] * right_pair[1] + left_pair[1] * right_pair[0],
    )


def conj_mul(left_pair, right_pair):
    return (
        left_pair[0] * right_pair[0] + left_pair[1] * right_pair[1],
        left_pair[0] * right_pair[1] - left_pair[1] * right_pair[0],
    )


def row_transform(data_pair, direction):
    batch_len, length, block_width = data_pair[0].shape
    outer_len, inner_len = split_factor(length)
    outer_ids = jnp.arange(outer_len, dtype=jnp.int32)
    inner_ids = jnp.arange(inner_len, dtype=jnp.int32)
    real_in = data_pair[0].reshape(batch_len, outer_len, inner_len, block_width)
    imag_in = None
    if data_pair[1] is not None:
        imag_in = data_pair[1].reshape(batch_len, outer_len, inner_len, block_width)
    middle = complex_einsum(
        "bjmc,jk->bkmc", (real_in, imag_in), phase_table(outer_ids, outer_ids, outer_len, direction)
    )
    twiddle = phase_table(outer_ids, inner_ids, length, direction)
    middle = complex_mul(middle, (twiddle[0][None, :, :, None], twiddle[1][None, :, :, None]))
    result = complex_einsum(
        "bkmc,mq->bqkc", middle, phase_table(inner_ids, inner_ids, inner_len, direction)
    )
    norm_factor = 1.0 if direction < 0 else 1.0 / length
    return (
        result[0].reshape(batch_len, length, block_width) * norm_factor,
        result[1].reshape(batch_len, length, block_width) * norm_factor,
    )


def block_order(groups, fields_count):
    positions = jnp.arange(groups, dtype=jnp.int32)
    blocks = positions % fields_count * (groups // fields_count) + positions // fields_count
    return (positions, blocks)


def column_forward(data_pair, groups, fields_count):
    batch_len, local_rows, total_len = data_pair[0].shape
    block_width = total_len // groups
    positions, blocks = block_order(groups, fields_count)
    column_ids = jnp.arange(block_width, dtype=jnp.int32)
    shaped = (
        data_pair[0].reshape(batch_len, local_rows, groups, block_width),
        data_pair[1].reshape(batch_len, local_rows, groups, block_width),
    )
    middle = complex_einsum("brpc,pk->brkc", shaped, phase_table(blocks, positions, groups, -1.0))
    twiddle = phase_table(positions, column_ids, total_len, -1.0)
    middle = complex_mul(middle, (twiddle[0][None, None], twiddle[1][None, None]))
    result = complex_einsum(
        "brkc,cq->brqk", middle, phase_table(column_ids, column_ids, block_width, -1.0)
    )
    return (
        result[0].reshape(batch_len, local_rows, total_len),
        result[1].reshape(batch_len, local_rows, total_len),
    )


def column_inverse(data_pair, groups, fields_count):
    batch_len, local_rows, total_len = data_pair[0].shape
    block_width = total_len // groups
    positions, blocks = block_order(groups, fields_count)
    column_ids = jnp.arange(block_width, dtype=jnp.int32)
    shaped = (
        data_pair[0].reshape(batch_len, local_rows, block_width, groups),
        data_pair[1].reshape(batch_len, local_rows, block_width, groups),
    )
    middle = complex_einsum(
        "brqk,qc->brkc", shaped, phase_table(column_ids, column_ids, block_width, 1.0)
    )
    twiddle = phase_table(positions, column_ids, total_len, 1.0)
    middle = complex_mul(middle, (twiddle[0][None, None], twiddle[1][None, None]))
    result = complex_einsum("brkc,kp->brpc", middle, phase_table(positions, blocks, groups, 1.0))
    norm_factor = 1.0 / total_len
    return (
        result[0].reshape(batch_len, local_rows, total_len) * norm_factor,
        result[1].reshape(batch_len, local_rows, total_len) * norm_factor,
    )


def body(sky_maps, band_cuts, filters, wiener, response):
    rows_count = lax.axis_size("rows")
    fields_count = lax.axis_size("fields")
    groups = rows_count * fields_count
    local_rows = filters.shape[1]
    total_rows = local_rows * groups
    row_ratio = NC // total_rows

    def forward_columns(stacked):
        return jnp.stack(column_forward((stacked[0], stacked[1]), groups, fields_count))

    def inverse_rows(stacked):
        return jnp.stack(row_transform((stacked[0], stacked[1]), 1.0))

    def inverse_columns(stacked):
        return jnp.stack(column_inverse((stacked[0], stacked[1]), groups, fields_count))

    def to_frequency(stacked):
        batch_len = stacked.shape[1]
        block_width = stacked.shape[3]
        shaped = stacked.reshape(
            2, batch_len, rows_count, fields_count, local_rows, 1, 1, block_width
        )
        arrived = lax.all_to_all(
            lax.all_to_all(shaped, "rows", split_axis=2, concat_axis=5, tiled=True),
            "fields",
            split_axis=3,
            concat_axis=6,
            tiled=True,
        )
        result = forward_columns(arrived.reshape(2, batch_len, local_rows, groups * block_width))
        return result

    def to_space(stacked):
        batch_len = stacked.shape[1]
        block_width = stacked.shape[3] // groups
        shaped = stacked.reshape(
            2, batch_len, 1, 1, local_rows, rows_count, fields_count, block_width
        )
        arrived = lax.all_to_all(
            lax.all_to_all(shaped, "rows", split_axis=5, concat_axis=2, tiled=True),
            "fields",
            split_axis=6,
            concat_axis=3,
            tiled=True,
        )
        result = inverse_rows(arrived.reshape(2, batch_len, total_rows, block_width))
        return result

    slab_spectra = jnp.stack(
        row_transform(
            (lax.all_to_all(sky_maps, "rows", split_axis=2, concat_axis=1, tiled=True), None), -1.0
        )
    )
    sky_spectra = to_frequency(slab_spectra)
    row_ids = lax.axis_index(("rows", "fields")) * local_rows + jnp.arange(
        local_rows, dtype=jnp.int32
    )
    freq_rows = jnp.where(row_ids < total_rows // 2, row_ids, row_ids - total_rows)[:, None]
    column_ids = jnp.arange(NC, dtype=jnp.int32)
    freq_cols = jnp.where(column_ids < NC // 2, column_ids, column_ids - NC)[None, :]
    scaled_rows = row_ratio * freq_rows
    radius_sq = freq_cols * freq_cols + scaled_rows * scaled_rows

    def band_mask(lower_cut, upper_cut):
        inside = (radius_sq >= lower_cut * lower_cut) & (radius_sq <= upper_cut * upper_cut)
        return inside.astype(jnp.float32)

    mask_temp = band_mask(band_cuts[0], band_cuts[1])
    mask_pol = band_mask(band_cuts[2], band_cuts[3])
    mask_out = band_mask(band_cuts[4], band_cuts[5])
    radius_floor = jnp.maximum(radius_sq, 1).astype(jnp.float32)
    cos_two = (freq_cols * freq_cols - scaled_rows * scaled_rows).astype(jnp.float32) / radius_floor
    sin_two = (2 * freq_cols * scaled_rows).astype(jnp.float32) / radius_floor
    along_x = (2 * freq_cols).astype(jnp.float32) / NC
    along_y = (2 * freq_rows).astype(jnp.float32) / total_rows
    raising = (-along_y + 0.0 * along_x, along_x + 0.0 * along_y)
    lowering = (along_y + 0.0 * along_x, along_x + 0.0 * along_y)
    rotation = (cos_two, sin_two)
    temp_modes = (sky_spectra[0, 0], sky_spectra[1, 0])
    stokes_q = (sky_spectra[0, 1], sky_spectra[1, 1])
    stokes_u = (sky_spectra[0, 2], sky_spectra[1, 2])
    e_modes = (
        -(cos_two * stokes_q[0] + sin_two * stokes_u[0]),
        -(cos_two * stokes_q[1] + sin_two * stokes_u[1]),
    )
    b_modes = (
        sin_two * stokes_q[0] - cos_two * stokes_u[0],
        sin_two * stokes_q[1] - cos_two * stokes_u[1],
    )
    temp_weight = mask_temp * filters[0]
    e_weight = mask_pol * filters[1]
    b_weight = mask_pol * filters[2]
    temp_bar = (temp_weight * temp_modes[0], temp_weight * temp_modes[1])
    e_bar = (e_weight * e_modes[0], e_weight * e_modes[1])
    b_bar = (b_weight * b_modes[0], b_weight * b_modes[1])
    grad_temp = complex_mul(raising, (wiener[0] * temp_bar[0], wiener[0] * temp_bar[1]))
    pol_sum = complex_mul((e_bar[0] - b_bar[1], e_bar[1] + b_bar[0]), rotation)
    pol_bar = (-pol_sum[0], -pol_sum[1])
    pol_rot = complex_mul((wiener[1] * e_bar[0], wiener[1] * e_bar[1]), rotation)
    pol_wiener = (-pol_rot[0], -pol_rot[1])
    spin_three = complex_mul(raising, pol_wiener)
    spin_one = complex_mul(lowering, pol_wiener)
    leg_spectra = jnp.stack(
        [
            jnp.stack([temp_bar[0], grad_temp[0], pol_bar[0], spin_three[0], spin_one[0]]),
            jnp.stack([temp_bar[1], grad_temp[1], pol_bar[1], spin_three[1], spin_one[1]]),
        ]
    )
    leg_maps = to_space(inverse_columns(leg_spectra))
    temp_leg = (leg_maps[0, 0], leg_maps[1, 0])
    grad_leg = (leg_maps[0, 1], leg_maps[1, 1])
    pol_leg = (leg_maps[0, 2], leg_maps[1, 2])
    three_leg = (leg_maps[0, 3], leg_maps[1, 3])
    one_leg = (leg_maps[0, 4], leg_maps[1, 4])
    temp_term = complex_mul(temp_leg, grad_leg)
    raise_term = conj_mul(pol_leg, three_leg)
    lower_term = conj_mul(one_leg, pol_leg)
    current = (
        temp_term[0] + 0.5 * (raise_term[0] + lower_term[0]),
        temp_term[1] + 0.5 * (raise_term[1] + lower_term[1]),
    )
    current_rows = jnp.stack(row_transform((current[0][None], current[1][None]), -1.0))
    current_modes = to_frequency(current_rows)
    out_weight = mask_out * response
    estimate_modes = complex_mul(
        lowering, (out_weight * current_modes[0, 0], out_weight * current_modes[1, 0])
    )
    estimate_stack = jnp.stack([estimate_modes[0][None], estimate_modes[1][None]])
    estimate_maps = to_space(inverse_columns(estimate_stack))
    slab_result = estimate_maps[:, 0]
    return lax.all_to_all(slab_result, "rows", split_axis=1, concat_axis=2, tiled=True)


SIDE = 128
TILE = (8, 128)
MESH = pl.DeviceIdType.MESH


def add_pair(a, b):
    imag = a[1] if b[1] is None else b[1] if a[1] is None else a[1] + b[1]
    return (a[0] + b[0], imag)


def sub_pair(a, b):
    imag = a[1] if b[1] is None else -b[1] if a[1] is None else a[1] - b[1]
    return (a[0] - b[0], imag)


def turn_pair(value, step, length, direction):
    real, imag = value
    if step == 0:
        return value
    if 4 * step == length:
        if imag is None:
            return (jnp.zeros_like(real), real if direction > 0 else -real)
        return (-imag, real) if direction > 0 else (imag, -real)
    angle = 2.0 * math.pi * step / length
    c, s = math.cos(angle), direction * math.sin(angle)
    if imag is None:
        return (real * c, real * s)
    if 8 * step == length:
        if direction > 0:
            return ((real - imag) * c, (real + imag) * c)
        return ((real + imag) * c, (imag - real) * c)
    if 8 * step == 3 * length:
        if direction > 0:
            return ((real + imag) * c, (imag - real) * c)
        return ((real - imag) * c, (real + imag) * c)
    return (real * c - imag * s, real * s + imag * c)


def short_transform(values, direction):
    length = len(values)
    if length == 1:
        return values
    even = short_transform(values[0::2], direction)
    odd = short_transform(values[1::2], direction)
    low, high = [], []
    for step in range(length // 2):
        turned = turn_pair(odd[step], step, length, direction)
        low.append(add_pair(even[step], turned))
        high.append(sub_pair(even[step], turned))
    return low + high


def split_number(x):
    top = x.astype(jnp.bfloat16)
    return top, (x - top.astype(jnp.float32)).astype(jnp.bfloat16)


def dot32(a, b):
    return jnp.dot(a, b, preferred_element_type=jnp.float32)


def matrix_left(table_ref, which, x):
    top, rest = split_number(x)
    m_top, m_rest = table_ref[which, 0], table_ref[which, 1]
    return dot32(m_top, top) + (dot32(m_top, rest) + dot32(m_rest, top))


def matrix_right(table_ref, which, x):
    top, rest = split_number(x)
    m_top, m_rest = table_ref[which, 0], table_ref[which, 1]
    return dot32(top, m_top) + (dot32(top, m_rest) + dot32(rest, m_top))


def lens_kernel(
    rows_count, fields_count, local_rows,
    cuts_ref, sky_ref, weight_ref, table_ref, twiddle_ref, out_ref,
    slab_out, slab_in, spec_out, spec_in, weights, legs_out, legs_in, maps, current,
    cur_out, cur_in, est_out, est_in, fin_out, fin_in,
    slab_sem, spec_sem, legs_sem, cur_sem, est_sem, fin_sem, self_sem,
):
    groups = rows_count * fields_count
    total_rows = groups * local_rows
    in_rows = total_rows // rows_count
    row_ratio = NC // total_rows
    my_r, my_f = lax.axis_index("rows"), lax.axis_index("fields")
    me = my_r * fields_count + my_f
    my_block = my_f * rows_count + my_r

    def place(index):
        return index // fields_count, index % fields_count

    def block_of(index):
        r, f = place(index)
        return f * rows_count + r

    def target(index):
        r, f = place(index)
        return {"rows": r, "fields": f}

    def send(q, src, dst, sems):
        peer = (me + q) % groups
        return pltpu.make_async_remote_copy(
            src_ref=src, dst_ref=dst, send_sem=sems[0], recv_sem=sems[1],
            device_id=target(peer), device_id_type=MESH,
        )

    def send_row(q, src, dst, sems):
        return pltpu.make_async_remote_copy(
            src_ref=src, dst_ref=dst, send_sem=sems[0], recv_sem=sems[1],
            device_id={"rows": (my_r + q) % rows_count}, device_id_type=MESH,
        )

    def each_peer(body, count=groups):
        def step(q, carry):
            body(q)
            return carry
        lax.fori_loop(1, count, step, 0)

    barrier = pltpu.get_barrier_semaphore()

    def greet(q):
        pl.semaphore_signal(
            barrier, inc=1, device_id=target((me + q) % groups), device_id_type=MESH
        )

    each_peer(greet)
    tiles = sky_ref.shape[2] // SIDE
    for field in range(3):
        for t in range(tiles):
            slab_out[t // 8, field, :, t % 8, :] = sky_ref[field, :, t * SIDE:(t + 1) * SIDE]
    pl.semaphore_wait(barrier, groups - 1)

    def slab_copy(q):
        return send_row(
            q, slab_out.at[(my_r + q) % rows_count], slab_in.at[my_r],
            (slab_sem.at[0, q], slab_sem.at[1, q]),
        )

    def slab_arrival(q):
        return send_row(
            q, slab_out.at[(my_r + q) % rows_count],
            slab_in.at[(my_r + rows_count - q) % rows_count],
            (slab_sem.at[0, q], slab_sem.at[1, q]),
        )

    each_peer(lambda q: slab_copy(q).start(), rows_count)
    own = pltpu.make_async_copy(slab_out.at[my_r], slab_in.at[my_r], self_sem.at[0])
    own.start()

    low_index = lax.broadcasted_iota(jnp.int32, (SIDE, SIDE), 0)
    high_index = lax.broadcasted_iota(jnp.int32, (SIDE, SIDE), 1)
    column_ids = low_index + SIDE * high_index
    freq_cols = jnp.where(column_ids < NC // 2, column_ids, column_ids - NC)

    def row_frequency(row):
        row_id = me * local_rows + row
        return jnp.where(row_id < total_rows // 2, row_id, row_id - total_rows)

    def weigh(row, carry):
        scaled = row_ratio * row_frequency(row)
        radius_sq = freq_cols * freq_cols + scaled * scaled

        def mask(n):
            low, high = cuts_ref[2 * n], cuts_ref[2 * n + 1]
            inside = (radius_sq >= low * low) & (radius_sq <= high * high)
            return inside.astype(jnp.float32)

        pol = mask(1)
        weights[0, row] = mask(0) * weight_ref[0, row].T
        weights[1, row] = pol * weight_ref[1, row].T
        weights[2, row] = pol * weight_ref[2, row].T
        weights[3, row] = weight_ref[3, row].T
        weights[4, row] = weight_ref[4, row].T
        weights[5, row] = mask(2) * weight_ref[5, row].T
        return carry

    lax.fori_loop(0, local_rows, weigh, 0)

    each_peer(lambda q: slab_arrival(q).wait_recv(), rows_count)
    own.wait()

    def spec_copy(field, q, src_block):
        peer = (me + q) % groups
        return send(
            q, spec_out.at[field, peer], spec_in.at[field, :, :, src_block],
            (spec_sem.at[0, field, q], spec_sem.at[1, field, q]),
        )

    def own_spec(field):
        return pltpu.make_async_copy(
            spec_out.at[field, me], spec_in.at[field, :, :, my_block], self_sem.at[1 + field]
        )

    def row_step(field, carry):
        values = [
            (slab_in[y // in_rows, field, y % in_rows], None) for y in range(total_rows)
        ]
        for k, (real, imag) in enumerate(short_transform(values, -1)):
            spec_out[field, k // local_rows, k % local_rows, 0] = real
            spec_out[field, k // local_rows, k % local_rows, 1] = (
                jnp.zeros_like(real) if imag is None else imag
            )
        each_peer(lambda q: spec_copy(field, q, my_block).start())
        own_spec(field).start()
        return carry

    lax.fori_loop(0, 3, row_step, 0)

    def row_wait(field, carry):
        each_peer(
            lambda q: spec_copy(field, q, block_of((me + groups - q) % groups)).wait_recv()
        )
        own_spec(field).wait()
        return carry

    lax.fori_loop(0, 3, row_wait, 0)

    cos_f, sin_f, cos_b, sin_b = 0, 1, 2, 3

    def long_forward(pieces):
        turned = []
        for piece in pieces:
            y = matrix_left(table_ref, 0, piece)
            yr, yi = y[:SIDE], y[SIDE:]
            c, s = twiddle_ref[cos_f], twiddle_ref[sin_f]
            z = jnp.concatenate([yr * c - yi * s, yr * s + yi * c], axis=1)
            z = matrix_right(table_ref, 1, z)
            turned.append((z[:, :SIDE], z[:, SIDE:]))
        return turned

    def long_inverse(pair):
        u = matrix_right(table_ref, 0, jnp.concatenate([pair[0], pair[1]], axis=1))
        ur, ui = u[:, :SIDE], u[:, SIDE:]
        c, s = twiddle_ref[cos_b], twiddle_ref[sin_b]
        v = jnp.concatenate([ur * c - ui * s, ur * s + ui * c], axis=0)
        return matrix_left(table_ref, 1, v)

    def legs_copy(row, q, src_index):
        peer = (me + q) % groups
        return send(
            q, legs_out.at[row, :, :, block_of(peer)], legs_in.at[row, src_index],
            (legs_sem.at[0, row, q], legs_sem.at[1, row, q]),
        )

    def own_legs(row):
        return pltpu.make_async_copy(
            legs_out.at[row, :, :, my_block], legs_in.at[row, me], self_sem.at[4 + row]
        )

    def slopes(row):
        along_x = (2 * freq_cols).astype(jnp.float32) / NC
        along_y = (2 * row_frequency(row)).astype(jnp.float32) / total_rows
        return along_x, along_y

    def leg_step(row, carry):
        temp, stokes_q, stokes_u = long_forward(
            [spec_in[field, row].reshape(2 * SIDE, SIDE) for field in range(3)]
        )
        scaled = row_ratio * row_frequency(row)
        radius_sq = freq_cols * freq_cols + scaled * scaled
        floor = jnp.maximum(radius_sq, 1).astype(jnp.float32)
        cos2 = (freq_cols * freq_cols - scaled * scaled).astype(jnp.float32) / floor
        sin2 = (2 * freq_cols * scaled).astype(jnp.float32) / floor
        along_x, along_y = slopes(row)
        raising, lowering = (-along_y, along_x), (along_y, along_x)
        rot = (cos2, sin2)
        w_t, w_e, w_b = weights[0, row], weights[1, row], weights[2, row]
        w_gt, w_ge = weights[3, row], weights[4, row]
        t_bar = (w_t * temp[0], w_t * temp[1])
        e_bar = tuple(-w_e * (cos2 * a + sin2 * b) for a, b in zip(stokes_q, stokes_u))
        b_bar = tuple(w_b * (sin2 * a - cos2 * b) for a, b in zip(stokes_q, stokes_u))
        g = complex_mul((w_gt * t_bar[0], w_gt * t_bar[1]), raising)
        p = complex_mul((b_bar[1] - e_bar[0], -(e_bar[1] + b_bar[0])), rot)
        w = complex_mul((-w_ge * e_bar[0], -w_ge * e_bar[1]), rot)
        h3 = complex_mul(w, raising)
        h1 = complex_mul(w, lowering)
        for n, leg in enumerate((t_bar, g, p, h3, h1)):
            legs_out[row, n] = long_inverse(leg).reshape((2, groups) + TILE)
        each_peer(lambda q: legs_copy(row, q, me).start())
        own_legs(row).start()
        return carry

    lax.fori_loop(0, local_rows, leg_step, 0)

    def leg_wait(row, carry):
        each_peer(lambda q: legs_copy(row, q, (me + groups - q) % groups).wait_recv())
        own_legs(row).wait()
        return carry

    lax.fori_loop(0, local_rows, leg_wait, 0)

    def map_step(n, carry):
        values = [
            (legs_in[k % local_rows, k // local_rows, n, 0],
             legs_in[k % local_rows, k // local_rows, n, 1])
            for k in range(total_rows)
        ]
        for y, (real, imag) in enumerate(short_transform(values, 1)):
            maps[n, 0, y] = real
            maps[n, 1, y] = imag
        return carry

    lax.fori_loop(0, 5, map_step, 0)

    def product_step(y, carry):
        a, g, p, h3, h1 = [(maps[n, 0, y], maps[n, 1, y]) for n in range(5)]
        ag, ph, hp = complex_mul(a, g), conj_mul(p, h3), conj_mul(h1, p)
        current[0, y] = ag[0] + 0.5 * (ph[0] + hp[0])
        current[1, y] = ag[1] + 0.5 * (ph[1] + hp[1])
        return carry

    lax.fori_loop(0, total_rows, product_step, 0)

    values = [(current[0, y], current[1, y]) for y in range(total_rows)]
    for k, (real, imag) in enumerate(short_transform(values, -1)):
        cur_out[k // local_rows, k % local_rows, 0] = real
        cur_out[k // local_rows, k % local_rows, 1] = imag

    def cur_copy(q, src_block):
        return send(
            q, cur_out.at[(me + q) % groups], cur_in.at[:, :, src_block],
            (cur_sem.at[0, q], cur_sem.at[1, q]),
        )

    each_peer(lambda q: cur_copy(q, my_block).start())
    own_cur = pltpu.make_async_copy(
        cur_out.at[me], cur_in.at[:, :, my_block], self_sem.at[4 + local_rows]
    )
    own_cur.start()
    each_peer(lambda q: cur_copy(q, block_of((me + groups - q) % groups)).wait_recv())
    own_cur.wait()

    def estimate_step(row, carry):
        (modes,) = long_forward([cur_in[row].reshape(2 * SIDE, SIDE)])
        along_x, along_y = slopes(row)
        w = weights[5, row]
        estimate = complex_mul((w * modes[0], w * modes[1]), (along_y, along_x))
        est_out[row] = long_inverse(estimate).reshape((2, groups) + TILE)
        return carry

    lax.fori_loop(0, local_rows, estimate_step, 0)

    def est_copy(q, src_index):
        return send(
            q, est_out.at[:, :, block_of((me + q) % groups)], est_in.at[src_index],
            (est_sem.at[0, q], est_sem.at[1, q]),
        )

    each_peer(lambda q: est_copy(q, me).start())
    own_est = pltpu.make_async_copy(
        est_out.at[:, :, my_block], est_in.at[me], self_sem.at[5 + local_rows]
    )
    own_est.start()
    each_peer(lambda q: est_copy(q, (me + groups - q) % groups).wait_recv())
    own_est.wait()

    values = [
        (est_in[k // local_rows, k % local_rows, 0], est_in[k // local_rows, k % local_rows, 1])
        for k in range(total_rows)
    ]
    for y, (real, imag) in enumerate(short_transform(values, 1)):
        fin_out[y // in_rows, 0, y % in_rows] = real
        fin_out[y // in_rows, 1, y % in_rows] = imag

    def fin_copy(q, src_row):
        return send_row(
            q, fin_out.at[(my_r + q) % rows_count], fin_in.at[src_row],
            (fin_sem.at[0, q], fin_sem.at[1, q]),
        )

    each_peer(lambda q: fin_copy(q, my_r).start(), rows_count)
    own_fin = pltpu.make_async_copy(
        fin_out.at[my_r], fin_in.at[my_r], self_sem.at[6 + local_rows]
    )
    own_fin.start()
    each_peer(
        lambda q: fin_copy(q, (my_r + rows_count - q) % rows_count).wait_recv(), rows_count
    )
    own_fin.wait()
    for part in range(2):
        for t in range(tiles):
            out_ref[part, :, t * SIDE:(t + 1) * SIDE] = fin_in[t // 8, part, :, t % 8, :]

    each_peer(lambda q: slab_copy(q).wait_send(), rows_count)

    def spec_left(field, carry):
        each_peer(lambda q: spec_copy(field, q, my_block).wait_send())
        return carry

    lax.fori_loop(0, 3, spec_left, 0)

    def legs_left(row, carry):
        each_peer(lambda q: legs_copy(row, q, me).wait_send())
        return carry

    lax.fori_loop(0, local_rows, legs_left, 0)
    each_peer(lambda q: cur_copy(q, my_block).wait_send())
    each_peer(lambda q: est_copy(q, me).wait_send())
    each_peer(lambda q: fin_copy(q, my_r).wait_send(), rows_count)


def long_tables(total_rows):
    index = np.arange(SIDE)
    angle = 2.0 * np.pi * (index[:, None] * index[None, :] % SIDE) / SIDE
    c, s = np.cos(angle), np.sin(angle)
    forward = np.block([[c, s], [-s, c]]).astype(np.float32)
    tables = np.stack([forward, forward.T])
    top = tables.astype(jnp.bfloat16)
    rest = (tables - top.astype(np.float32)).astype(jnp.bfloat16)
    turn = 2.0 * np.pi * (index[:, None] * index[None, :]) / NC
    scale = 1.0 / (NC * total_rows)
    twiddle = np.stack(
        [np.cos(turn), -np.sin(turn), scale * np.cos(turn), scale * np.sin(turn)]
    ).astype(np.float32)
    return np.stack([top, rest], axis=1), twiddle


def fused_body(rows_count, fields_count, sky_maps, band_cuts, filters, wiener, response):
    groups = rows_count * fields_count
    local_rows = response.shape[0]
    total_rows = local_rows * groups
    in_rows = total_rows // rows_count
    table, twiddle = long_tables(total_rows)
    weight = jnp.concatenate([filters, wiener, response[None]]).reshape(
        6, local_rows, SIDE, SIDE
    )
    vmem = pl.BlockSpec(memory_space=pltpu.VMEM)
    f32 = jnp.float32
    dma = pltpu.SemaphoreType.DMA
    slab = pltpu.VMEM((rows_count, 3, in_rows) + TILE, f32)
    chunk = pltpu.VMEM((groups, local_rows, 2) + TILE, f32)
    lines = pltpu.VMEM((local_rows, 2, groups) + TILE, f32)
    final = pltpu.VMEM((rows_count, 2, in_rows) + TILE, f32)
    return pl.pallas_call(
        functools.partial(lens_kernel, rows_count, fields_count, local_rows),
        out_shape=jax.ShapeDtypeStruct((2,) + sky_maps.shape[1:], f32),
        in_specs=[pl.BlockSpec(memory_space=pltpu.SMEM)] + [vmem] * 4,
        out_specs=vmem,
        scratch_shapes=[
            slab, slab,
            pltpu.VMEM((3, groups, local_rows, 2) + TILE, f32),
            pltpu.VMEM((3, local_rows, 2, groups) + TILE, f32),
            pltpu.VMEM((6, local_rows, SIDE, SIDE), f32),
            pltpu.VMEM((local_rows, 5, 2, groups) + TILE, f32),
            pltpu.VMEM((local_rows, groups, 5, 2) + TILE, f32),
            pltpu.VMEM((5, 2, total_rows) + TILE, f32),
            pltpu.VMEM((2, total_rows) + TILE, f32),
            chunk, lines, lines, chunk, final, final,
            dma((2, rows_count)), dma((2, 3, groups)), dma((2, local_rows, groups)),
            dma((2, groups)), dma((2, groups)), dma((2, rows_count)), dma((7 + local_rows,)),
        ],
        compiler_params=pltpu.CompilerParams(
            collective_id=0, has_side_effects=True, vmem_limit_bytes=48 * 1024 * 1024
        ),
        name="lens",
    )(band_cuts, sky_maps, weight, jnp.asarray(table), jnp.asarray(twiddle))


def solution(mesh):
    placed = (
        P("sims", "rows", "fields"),
        P(),
        P(None, ("rows", "fields"), None),
        P(None, ("rows", "fields"), None),
        P(("rows", "fields"), None),
    )
    rows_count, fields_count = mesh.shape["rows"], mesh.shape["fields"]
    groups = rows_count * fields_count

    def choose(sky_maps, *rest):
        fits = (
            NC == SIDE * SIDE
            and NC // groups == TILE[0] * TILE[1]
            and sky_maps.shape[1] % 8 == 0
            and sky_maps.shape[1] * rows_count in (16, 32, 64)
        )
        if fits:
            return fused_body(rows_count, fields_count, sky_maps, *rest)
        return body(sky_maps, *rest)

    return jax.shard_map(
        choose, mesh=mesh, in_specs=placed, out_specs=P("sims", "rows", "fields"), check_vma=False
    )
```

```python
import functools
import math

import jax
import jax.numpy as jnp
import numpy as np
from jax import lax
from jax.experimental import pallas as pl
from jax.experimental.pallas import tpu as pltpu
from jax.sharding import PartitionSpec as P

NC = 16384


exact_mode = lax.Precision.HIGHEST


def split_factor(length):
    best_first = 1
    for divisor in range(1, math.isqrt(length) + 1):
        if length % divisor == 0:
            best_first = divisor
    return (best_first, length // best_first)


def phase_table(left_index, right_index, period, direction):
    product = left_index[:, None] * right_index[None, :] % period
    angles = direction * 2.0 * math.pi / period * product.astype(jnp.float32)
    return (jnp.cos(angles), jnp.sin(angles))


def complex_einsum(formula, data_pair, table_pair):
    data_real, data_imag = data_pair
    table_real, table_imag = table_pair
    real_out = jnp.einsum(formula, data_real, table_real, precision=exact_mode)
    imag_out = jnp.einsum(formula, data_real, table_imag, precision=exact_mode)
    if data_imag is not None:
        real_out = real_out - jnp.einsum(formula, data_imag, table_imag, precision=exact_mode)
        imag_out = imag_out + jnp.einsum(formula, data_imag, table_real, precision=exact_mode)
    return (real_out, imag_out)


def complex_mul(left_pair, right_pair):
    return (
        left_pair[0] * right_pair[0] - left_pair[1] * right_pair[1],
        left_pair[0] * right_pair[1] + left_pair[1] * right_pair[0],
    )


def conj_mul(left_pair, right_pair):
    return (
        left_pair[0] * right_pair[0] + left_pair[1] * right_pair[1],
        left_pair[0] * right_pair[1] - left_pair[1] * right_pair[0],
    )


def row_transform(data_pair, direction):
    batch_len, length, block_width = data_pair[0].shape
    outer_len, inner_len = split_factor(length)
    outer_ids = jnp.arange(outer_len, dtype=jnp.int32)
    inner_ids = jnp.arange(inner_len, dtype=jnp.int32)
    real_in = data_pair[0].reshape(batch_len, outer_len, inner_len, block_width)
    imag_in = None
    if data_pair[1] is not None:
        imag_in = data_pair[1].reshape(batch_len, outer_len, inner_len, block_width)
    middle = complex_einsum(
        "bjmc,jk->bkmc", (real_in, imag_in), phase_table(outer_ids, outer_ids, outer_len, direction)
    )
    twiddle = phase_table(outer_ids, inner_ids, length, direction)
    middle = complex_mul(middle, (twiddle[0][None, :, :, None], twiddle[1][None, :, :, None]))
    result = complex_einsum(
        "bkmc,mq->bqkc", middle, phase_table(inner_ids, inner_ids, inner_len, direction)
    )
    norm_factor = 1.0 if direction < 0 else 1.0 / length
    return (
        result[0].reshape(batch_len, length, block_width) * norm_factor,
        result[1].reshape(batch_len, length, block_width) * norm_factor,
    )


def block_order(groups, fields_count):
    positions = jnp.arange(groups, dtype=jnp.int32)
    blocks = positions % fields_count * (groups // fields_count) + positions // fields_count
    return (positions, blocks)


def column_forward(data_pair, groups, fields_count):
    batch_len, local_rows, total_len = data_pair[0].shape
    block_width = total_len // groups
    positions, blocks = block_order(groups, fields_count)
    column_ids = jnp.arange(block_width, dtype=jnp.int32)
    shaped = (
        data_pair[0].reshape(batch_len, local_rows, groups, block_width),
        data_pair[1].reshape(batch_len, local_rows, groups, block_width),
    )
    middle = complex_einsum("brpc,pk->brkc", shaped, phase_table(blocks, positions, groups, -1.0))
    twiddle = phase_table(positions, column_ids, total_len, -1.0)
    middle = complex_mul(middle, (twiddle[0][None, None], twiddle[1][None, None]))
    result = complex_einsum(
        "brkc,cq->brqk", middle, phase_table(column_ids, column_ids, block_width, -1.0)
    )
    return (
        result[0].reshape(batch_len, local_rows, total_len),
        result[1].reshape(batch_len, local_rows, total_len),
    )


def column_inverse(data_pair, groups, fields_count):
    batch_len, local_rows, total_len = data_pair[0].shape
    block_width = total_len // groups
    positions, blocks = block_order(groups, fields_count)
    column_ids = jnp.arange(block_width, dtype=jnp.int32)
    shaped = (
        data_pair[0].reshape(batch_len, local_rows, block_width, groups),
        data_pair[1].reshape(batch_len, local_rows, block_width, groups),
    )
    middle = complex_einsum(
        "brqk,qc->brkc", shaped, phase_table(column_ids, column_ids, block_width, 1.0)
    )
    twiddle = phase_table(positions, column_ids, total_len, 1.0)
    middle = complex_mul(middle, (twiddle[0][None, None], twiddle[1][None, None]))
    result = complex_einsum("brkc,kp->brpc", middle, phase_table(positions, blocks, groups, 1.0))
    norm_factor = 1.0 / total_len
    return (
        result[0].reshape(batch_len, local_rows, total_len) * norm_factor,
        result[1].reshape(batch_len, local_rows, total_len) * norm_factor,
    )


def body(sky_maps, band_cuts, filters, wiener, response):
    rows_count = lax.axis_size("rows")
    fields_count = lax.axis_size("fields")
    groups = rows_count * fields_count
    local_rows = filters.shape[1]
    total_rows = local_rows * groups
    row_ratio = NC // total_rows

    def forward_columns(stacked):
        return jnp.stack(column_forward((stacked[0], stacked[1]), groups, fields_count))

    def inverse_rows(stacked):
        return jnp.stack(row_transform((stacked[0], stacked[1]), 1.0))

    def inverse_columns(stacked):
        return jnp.stack(column_inverse((stacked[0], stacked[1]), groups, fields_count))

    def to_frequency(stacked):
        batch_len = stacked.shape[1]
        block_width = stacked.shape[3]
        shaped = stacked.reshape(
            2, batch_len, rows_count, fields_count, local_rows, 1, 1, block_width
        )
        arrived = lax.all_to_all(
            lax.all_to_all(shaped, "rows", split_axis=2, concat_axis=5, tiled=True),
            "fields",
            split_axis=3,
            concat_axis=6,
            tiled=True,
        )
        result = forward_columns(arrived.reshape(2, batch_len, local_rows, groups * block_width))
        return result

    def to_space(stacked):
        batch_len = stacked.shape[1]
        block_width = stacked.shape[3] // groups
        shaped = stacked.reshape(
            2, batch_len, 1, 1, local_rows, rows_count, fields_count, block_width
        )
        arrived = lax.all_to_all(
            lax.all_to_all(shaped, "rows", split_axis=5, concat_axis=2, tiled=True),
            "fields",
            split_axis=6,
            concat_axis=3,
            tiled=True,
        )
        result = inverse_rows(arrived.reshape(2, batch_len, total_rows, block_width))
        return result

    slab_spectra = jnp.stack(
        row_transform(
            (lax.all_to_all(sky_maps, "rows", split_axis=2, concat_axis=1, tiled=True), None), -1.0
        )
    )
    sky_spectra = to_frequency(slab_spectra)
    row_ids = lax.axis_index(("rows", "fields")) * local_rows + jnp.arange(
        local_rows, dtype=jnp.int32
    )
    freq_rows = jnp.where(row_ids < total_rows // 2, row_ids, row_ids - total_rows)[:, None]
    column_ids = jnp.arange(NC, dtype=jnp.int32)
    freq_cols = jnp.where(column_ids < NC // 2, column_ids, column_ids - NC)[None, :]
    scaled_rows = row_ratio * freq_rows
    radius_sq = freq_cols * freq_cols + scaled_rows * scaled_rows

    def band_mask(lower_cut, upper_cut):
        inside = (radius_sq >= lower_cut * lower_cut) & (radius_sq <= upper_cut * upper_cut)
        return inside.astype(jnp.float32)

    mask_temp = band_mask(band_cuts[0], band_cuts[1])
    mask_pol = band_mask(band_cuts[2], band_cuts[3])
    mask_out = band_mask(band_cuts[4], band_cuts[5])
    radius_floor = jnp.maximum(radius_sq, 1).astype(jnp.float32)
    cos_two = (freq_cols * freq_cols - scaled_rows * scaled_rows).astype(jnp.float32) / radius_floor
    sin_two = (2 * freq_cols * scaled_rows).astype(jnp.float32) / radius_floor
    along_x = (2 * freq_cols).astype(jnp.float32) / NC
    along_y = (2 * freq_rows).astype(jnp.float32) / total_rows
    raising = (-along_y + 0.0 * along_x, along_x + 0.0 * along_y)
    lowering = (along_y + 0.0 * along_x, along_x + 0.0 * along_y)
    rotation = (cos_two, sin_two)
    temp_modes = (sky_spectra[0, 0], sky_spectra[1, 0])
    stokes_q = (sky_spectra[0, 1], sky_spectra[1, 1])
    stokes_u = (sky_spectra[0, 2], sky_spectra[1, 2])
    e_modes = (
        -(cos_two * stokes_q[0] + sin_two * stokes_u[0]),
        -(cos_two * stokes_q[1] + sin_two * stokes_u[1]),
    )
    b_modes = (
        sin_two * stokes_q[0] - cos_two * stokes_u[0],
        sin_two * stokes_q[1] - cos_two * stokes_u[1],
    )
    temp_weight = mask_temp * filters[0]
    e_weight = mask_pol * filters[1]
    b_weight = mask_pol * filters[2]
    temp_bar = (temp_weight * temp_modes[0], temp_weight * temp_modes[1])
    e_bar = (e_weight * e_modes[0], e_weight * e_modes[1])
    b_bar = (b_weight * b_modes[0], b_weight * b_modes[1])
    grad_temp = complex_mul(raising, (wiener[0] * temp_bar[0], wiener[0] * temp_bar[1]))
    pol_sum = complex_mul((e_bar[0] - b_bar[1], e_bar[1] + b_bar[0]), rotation)
    pol_bar = (-pol_sum[0], -pol_sum[1])
    pol_rot = complex_mul((wiener[1] * e_bar[0], wiener[1] * e_bar[1]), rotation)
    pol_wiener = (-pol_rot[0], -pol_rot[1])
    spin_three = complex_mul(raising, pol_wiener)
    spin_one = complex_mul(lowering, pol_wiener)
    leg_spectra = jnp.stack(
        [
            jnp.stack([temp_bar[0], grad_temp[0], pol_bar[0], spin_three[0], spin_one[0]]),
            jnp.stack([temp_bar[1], grad_temp[1], pol_bar[1], spin_three[1], spin_one[1]]),
        ]
    )
    leg_maps = to_space(inverse_columns(leg_spectra))
    temp_leg = (leg_maps[0, 0], leg_maps[1, 0])
    grad_leg = (leg_maps[0, 1], leg_maps[1, 1])
    pol_leg = (leg_maps[0, 2], leg_maps[1, 2])
    three_leg = (leg_maps[0, 3], leg_maps[1, 3])
    one_leg = (leg_maps[0, 4], leg_maps[1, 4])
    temp_term = complex_mul(temp_leg, grad_leg)
    raise_term = conj_mul(pol_leg, three_leg)
    lower_term = conj_mul(one_leg, pol_leg)
    current = (
        temp_term[0] + 0.5 * (raise_term[0] + lower_term[0]),
        temp_term[1] + 0.5 * (raise_term[1] + lower_term[1]),
    )
    current_rows = jnp.stack(row_transform((current[0][None], current[1][None]), -1.0))
    current_modes = to_frequency(current_rows)
    out_weight = mask_out * response
    estimate_modes = complex_mul(
        lowering, (out_weight * current_modes[0, 0], out_weight * current_modes[1, 0])
    )
    estimate_stack = jnp.stack([estimate_modes[0][None], estimate_modes[1][None]])
    estimate_maps = to_space(inverse_columns(estimate_stack))
    slab_result = estimate_maps[:, 0]
    return lax.all_to_all(slab_result, "rows", split_axis=1, concat_axis=2, tiled=True)


SIDE = 128
TILE = (8, 128)
LEG_GROUPS = ((0, 2), (2, 2), (4, 1))
MESH = pl.DeviceIdType.MESH


def add_pair(a, b):
    imag = a[1] if b[1] is None else b[1] if a[1] is None else a[1] + b[1]
    return (a[0] + b[0], imag)


def sub_pair(a, b):
    imag = a[1] if b[1] is None else -b[1] if a[1] is None else a[1] - b[1]
    return (a[0] - b[0], imag)


def turn_pair(value, step, length, direction):
    real, imag = value
    if step == 0:
        return value
    if 4 * step == length:
        if imag is None:
            return (jnp.zeros_like(real), real if direction > 0 else -real)
        return (-imag, real) if direction > 0 else (imag, -real)
    angle = 2.0 * math.pi * step / length
    c, s = math.cos(angle), direction * math.sin(angle)
    if imag is None:
        return (real * c, real * s)
    if 8 * step == length:
        if direction > 0:
            return ((real - imag) * c, (real + imag) * c)
        return ((real + imag) * c, (imag - real) * c)
    if 8 * step == 3 * length:
        if direction > 0:
            return ((real + imag) * c, (imag - real) * c)
        return ((real - imag) * c, (real + imag) * c)
    return (real * c - imag * s, real * s + imag * c)


def short_transform(values, direction):
    length = len(values)
    if length == 1:
        return values
    even = short_transform(values[0::2], direction)
    odd = short_transform(values[1::2], direction)
    low, high = [], []
    for step in range(length // 2):
        turned = turn_pair(odd[step], step, length, direction)
        low.append(add_pair(even[step], turned))
        high.append(sub_pair(even[step], turned))
    return low + high


def split_number(x):
    top = x.astype(jnp.bfloat16)
    return top, (x - top.astype(jnp.float32)).astype(jnp.bfloat16)


def dot32(a, b):
    return jnp.dot(a, b, preferred_element_type=jnp.float32)


def matrix_left(table_ref, which, x):
    top, rest = split_number(x)
    m_top, m_rest = table_ref[which, 0], table_ref[which, 1]
    return dot32(m_top, top) + (dot32(m_top, rest) + dot32(m_rest, top))


def matrix_right(table_ref, which, x):
    top, rest = split_number(x)
    m_top, m_rest = table_ref[which, 0], table_ref[which, 1]
    return dot32(top, m_top) + (dot32(top, m_rest) + dot32(rest, m_top))


def lens_kernel(
    rows_count, fields_count, local_rows,
    cuts_ref, sky_ref, weight_ref, table_ref, twiddle_ref, out_ref,
    slab_out, slab_in, spec_out, spec_in, weights, legs_out, legs_in, maps, current,
    cur_out, cur_in, est_out, est_in, fin_out, fin_in,
    slab_sem, spec_sem, legs_sem, cur_sem, est_sem, fin_sem, self_sem,
):
    groups = rows_count * fields_count
    total_rows = groups * local_rows
    in_rows = total_rows // rows_count
    row_ratio = NC // total_rows
    my_r, my_f = lax.axis_index("rows"), lax.axis_index("fields")
    me = my_r * fields_count + my_f
    my_block = my_f * rows_count + my_r

    def place(index):
        return index // fields_count, index % fields_count

    def block_of(index):
        r, f = place(index)
        return f * rows_count + r

    def target(index):
        r, f = place(index)
        return {"rows": r, "fields": f}

    half = fields_count // 2
    my_half, my_spot = my_f // half, my_f % half

    def partner(q, sign):
        side = (my_half + 1 - q // (rows_count * half)) % 2
        spot = (my_spot + half + sign * ((q // rows_count + 1) % half)) % half
        r = (my_r + rows_count + sign * ((q + 1) % rows_count)) % rows_count
        return r * fields_count + side * half + spot

    def peer_of(q):
        return partner(q, 1)

    def source_of(q):
        return partner(q, -1)

    def send(q, src, dst, sems):
        return pltpu.make_async_remote_copy(
            src_ref=src, dst_ref=dst, send_sem=sems[0], recv_sem=sems[1],
            device_id=target(peer_of(q)), device_id_type=MESH,
        )

    def send_row(q, src, dst, sems):
        return pltpu.make_async_remote_copy(
            src_ref=src, dst_ref=dst, send_sem=sems[0], recv_sem=sems[1],
            device_id={"rows": (my_r + q) % rows_count}, device_id_type=MESH,
        )

    def each_peer(body):
        def step(q, carry):
            body(q)
            return carry
        lax.fori_loop(0, groups - 1, step, 0)

    def each_row_peer(body):
        for q in range(1, rows_count):
            body(q)

    barrier = pltpu.get_barrier_semaphore()

    def greet(q):
        pl.semaphore_signal(
            barrier, inc=1, device_id=target(peer_of(q)), device_id_type=MESH
        )

    each_peer(greet)
    tiles = sky_ref.shape[2] // SIDE
    for field in range(3):
        for t in range(tiles):
            slab_out[t // 8, field, :, t % 8, :] = sky_ref[field, :, t * SIDE:(t + 1) * SIDE]
    pl.semaphore_wait(barrier, groups - 1)

    def slab_copy(field, q, src_row):
        return send_row(
            q, slab_out.at[(my_r + q) % rows_count, field], slab_in.at[src_row, field],
            (slab_sem.at[0, field, q], slab_sem.at[1, field, q]),
        )

    def own_slab(field):
        return pltpu.make_async_copy(
            slab_out.at[my_r, field], slab_in.at[my_r, field], self_sem.at[field]
        )

    for field in range(3):
        each_row_peer(lambda q: slab_copy(field, q, my_r).start())
        own_slab(field).start()

    low_index = lax.broadcasted_iota(jnp.int32, (SIDE, SIDE), 0)
    high_index = lax.broadcasted_iota(jnp.int32, (SIDE, SIDE), 1)
    column_ids = low_index + SIDE * high_index
    freq_cols = jnp.where(column_ids < NC // 2, column_ids, column_ids - NC)

    def row_frequency(row):
        row_id = me * local_rows + row
        return jnp.where(row_id < total_rows // 2, row_id, row_id - total_rows)

    def weigh(row, carry):
        scaled = row_ratio * row_frequency(row)
        radius_sq = freq_cols * freq_cols + scaled * scaled

        def mask(n):
            low, high = cuts_ref[2 * n], cuts_ref[2 * n + 1]
            inside = (radius_sq >= low * low) & (radius_sq <= high * high)
            return inside.astype(jnp.float32)

        pol = mask(1)
        weights[0, row] = mask(0) * weight_ref[0, row].T
        weights[1, row] = pol * weight_ref[1, row].T
        weights[2, row] = pol * weight_ref[2, row].T
        weights[3, row] = weight_ref[3, row].T
        weights[4, row] = weight_ref[4, row].T
        weights[5, row] = mask(2) * weight_ref[5, row].T
        return carry

    lax.fori_loop(0, local_rows, weigh, 0)

    def spec_copy(field, row, q, src_block):
        return send(
            q, spec_out.at[field, row, peer_of(q)], spec_in.at[field, row, :, src_block],
            (spec_sem.at[0, field, row, q], spec_sem.at[1, field, row, q]),
        )

    def own_spec(field, row):
        return pltpu.make_async_copy(
            spec_out.at[field, row, me], spec_in.at[field, row, :, my_block],
            self_sem.at[3 + field * local_rows + row],
        )

    def spec_start(field, row):
        each_peer(lambda q: spec_copy(field, row, q, my_block).start())
        own_spec(field, row).start()

    def row_step(field, carry):
        each_row_peer(
            lambda q: slab_copy(field, q, (my_r + rows_count - q) % rows_count).wait_recv()
        )
        own_slab(field).wait()
        values = [
            (slab_in[y // in_rows, field, y % in_rows], None) for y in range(total_rows)
        ]
        for k, (real, imag) in enumerate(short_transform(values, -1)):
            spec_out[field, k % local_rows, k // local_rows, 0] = real
            spec_out[field, k % local_rows, k // local_rows, 1] = (
                jnp.zeros_like(real) if imag is None else imag
            )
        spec_start(field, 0)
        return carry

    lax.fori_loop(0, 3, row_step, 0)

    def later_rows(n, carry):
        spec_start(n % 3, 1 + n // 3)
        return carry

    lax.fori_loop(0, 3 * (local_rows - 1), later_rows, 0)

    def spec_wait(row):
        def step(field, carry):
            each_peer(lambda q: spec_copy(field, row, q, block_of(source_of(q))).wait_recv())
            own_spec(field, row).wait()
            return carry

        lax.fori_loop(0, 3, step, 0)

    cos_f, sin_f, cos_b, sin_b = 0, 1, 2, 3

    def side_by_side(pieces, axis):
        return pieces[0] if len(pieces) == 1 else jnp.concatenate(pieces, axis=axis)

    def long_forward(pieces):
        y = matrix_left(table_ref, 0, side_by_side(pieces, 1))
        c, s = twiddle_ref[cos_f], twiddle_ref[sin_f]
        turned = []
        for n in range(len(pieces)):
            yr, yi = y[:SIDE, n * SIDE:(n + 1) * SIDE], y[SIDE:, n * SIDE:(n + 1) * SIDE]
            turned.append(jnp.concatenate([yr * c - yi * s, yr * s + yi * c], axis=1))
        z = matrix_right(table_ref, 1, side_by_side(turned, 0))
        return [
            (z[n * SIDE:(n + 1) * SIDE, :SIDE], z[n * SIDE:(n + 1) * SIDE, SIDE:])
            for n in range(len(pieces))
        ]

    def long_inverse(pairs):
        stacks = [jnp.concatenate([pair[0], pair[1]], axis=1) for pair in pairs]
        u = matrix_right(table_ref, 0, side_by_side(stacks, 0))
        c, s = twiddle_ref[cos_b], twiddle_ref[sin_b]
        turned = []
        for n in range(len(pairs)):
            ur, ui = u[n * SIDE:(n + 1) * SIDE, :SIDE], u[n * SIDE:(n + 1) * SIDE, SIDE:]
            turned.append(jnp.concatenate([ur * c - ui * s, ur * s + ui * c], axis=0))
        x = matrix_left(table_ref, 1, side_by_side(turned, 1))
        return [
            x[:, n * SIDE:(n + 1) * SIDE].reshape((2, groups) + TILE)
            for n in range(len(pairs))
        ]

    leg_self = 3 + 3 * local_rows

    def legs_copy(row, g, q, src_index):
        first, count = LEG_GROUPS[g]
        return send(
            q, legs_out.at[row, first:first + count, :, block_of(peer_of(q))],
            legs_in.at[row, src_index, first:first + count],
            (legs_sem.at[0, row, g, q], legs_sem.at[1, row, g, q]),
        )

    def own_legs(row, g):
        first, count = LEG_GROUPS[g]
        return pltpu.make_async_copy(
            legs_out.at[row, first:first + count, :, my_block],
            legs_in.at[row, me, first:first + count],
            self_sem.at[leg_self + row * len(LEG_GROUPS) + g],
        )

    def slopes(row):
        along_x = (2 * freq_cols).astype(jnp.float32) / NC
        along_y = (2 * row_frequency(row)).astype(jnp.float32) / total_rows
        return along_x, along_y

    def leg_step(row, carry):
        spec_wait(row)
        temp, stokes_q, stokes_u = long_forward(
            [spec_in[field, row].reshape(2 * SIDE, SIDE) for field in range(3)]
        )
        scaled = row_ratio * row_frequency(row)
        radius_sq = freq_cols * freq_cols + scaled * scaled
        floor = jnp.maximum(radius_sq, 1).astype(jnp.float32)
        cos2 = (freq_cols * freq_cols - scaled * scaled).astype(jnp.float32) / floor
        sin2 = (2 * freq_cols * scaled).astype(jnp.float32) / floor
        along_x, along_y = slopes(row)
        raising, lowering = (-along_y, along_x), (along_y, along_x)
        rot = (cos2, sin2)
        w_t, w_e, w_b = weights[0, row], weights[1, row], weights[2, row]
        w_gt, w_ge = weights[3, row], weights[4, row]
        t_bar = (w_t * temp[0], w_t * temp[1])
        e_bar = tuple(-w_e * (cos2 * a + sin2 * b) for a, b in zip(stokes_q, stokes_u))
        b_bar = tuple(w_b * (sin2 * a - cos2 * b) for a, b in zip(stokes_q, stokes_u))
        g = complex_mul((w_gt * t_bar[0], w_gt * t_bar[1]), raising)
        p = complex_mul((b_bar[1] - e_bar[0], -(e_bar[1] + b_bar[0])), rot)
        w = complex_mul((-w_ge * e_bar[0], -w_ge * e_bar[1]), rot)
        h3 = complex_mul(w, raising)
        h1 = complex_mul(w, lowering)
        legs = (t_bar, g, p, h3, h1)
        for n, (first, count) in enumerate(LEG_GROUPS):
            for k, leg_map in enumerate(long_inverse(legs[first:first + count])):
                legs_out[row, first + k] = leg_map
            each_peer(lambda q: legs_copy(row, n, q, me).start())
            own_legs(row, n).start()
        return carry

    lax.fori_loop(0, local_rows, leg_step, 0)

    def leg_wait(g):
        def step(row, carry):
            each_peer(lambda q: legs_copy(row, g, q, source_of(q)).wait_recv())
            own_legs(row, g).wait()
            return carry

        lax.fori_loop(0, local_rows, step, 0)

    def map_step(n, carry):
        values = [
            (legs_in[k % local_rows, k // local_rows, n, 0],
             legs_in[k % local_rows, k // local_rows, n, 1])
            for k in range(total_rows)
        ]
        for y, (real, imag) in enumerate(short_transform(values, 1)):
            maps[n, 0, y] = real
            maps[n, 1, y] = imag
        return carry

    for g, (first, count) in enumerate(LEG_GROUPS):
        leg_wait(g)
        lax.fori_loop(first, first + count, map_step, 0)

    def product_step(y, carry):
        a, g, p, h3, h1 = [(maps[n, 0, y], maps[n, 1, y]) for n in range(5)]
        ag, ph, hp = complex_mul(a, g), conj_mul(p, h3), conj_mul(h1, p)
        current[0, y] = ag[0] + 0.5 * (ph[0] + hp[0])
        current[1, y] = ag[1] + 0.5 * (ph[1] + hp[1])
        return carry

    lax.fori_loop(0, total_rows, product_step, 0)

    values = [(current[0, y], current[1, y]) for y in range(total_rows)]
    for k, (real, imag) in enumerate(short_transform(values, -1)):
        cur_out[k % local_rows, k // local_rows, 0] = real
        cur_out[k % local_rows, k // local_rows, 1] = imag
    cur_self = leg_self + len(LEG_GROUPS) * local_rows
    est_self = cur_self + local_rows

    def cur_copy(row, q, src_block):
        return send(
            q, cur_out.at[row, peer_of(q)], cur_in.at[row, :, src_block],
            (cur_sem.at[0, row, q], cur_sem.at[1, row, q]),
        )

    def own_cur(row):
        return pltpu.make_async_copy(
            cur_out.at[row, me], cur_in.at[row, :, my_block], self_sem.at[cur_self + row]
        )

    def cur_start(row, carry):
        each_peer(lambda q: cur_copy(row, q, my_block).start())
        own_cur(row).start()
        return carry

    lax.fori_loop(0, local_rows, cur_start, 0)

    def est_copy(row, q, src_index):
        return send(
            q, est_out.at[row, :, block_of(peer_of(q))], est_in.at[row, src_index],
            (est_sem.at[0, row, q], est_sem.at[1, row, q]),
        )

    def own_est(row):
        return pltpu.make_async_copy(
            est_out.at[row, :, my_block], est_in.at[row, me], self_sem.at[est_self + row]
        )

    def estimate_step(row, carry):
        each_peer(lambda q: cur_copy(row, q, block_of(source_of(q))).wait_recv())
        own_cur(row).wait()
        (modes,) = long_forward([cur_in[row].reshape(2 * SIDE, SIDE)])
        along_x, along_y = slopes(row)
        w = weights[5, row]
        estimate = complex_mul((w * modes[0], w * modes[1]), (along_y, along_x))
        (est_out[row],) = long_inverse([estimate])
        each_peer(lambda q: est_copy(row, q, me).start())
        own_est(row).start()
        return carry

    lax.fori_loop(0, local_rows, estimate_step, 0)

    def est_wait(row, carry):
        each_peer(lambda q: est_copy(row, q, source_of(q)).wait_recv())
        own_est(row).wait()
        return carry

    lax.fori_loop(0, local_rows, est_wait, 0)

    values = [
        (est_in[k % local_rows, k // local_rows, 0], est_in[k % local_rows, k // local_rows, 1])
        for k in range(total_rows)
    ]
    for y, (real, imag) in enumerate(short_transform(values, 1)):
        fin_out[y // in_rows, 0, y % in_rows] = real
        fin_out[y // in_rows, 1, y % in_rows] = imag

    def fin_copy(q, src_row):
        return send_row(
            q, fin_out.at[(my_r + q) % rows_count], fin_in.at[src_row],
            (fin_sem.at[0, q], fin_sem.at[1, q]),
        )

    each_row_peer(lambda q: fin_copy(q, my_r).start())
    own_fin = pltpu.make_async_copy(
        fin_out.at[my_r], fin_in.at[my_r], self_sem.at[est_self + local_rows]
    )
    own_fin.start()
    each_row_peer(lambda q: fin_copy(q, (my_r + rows_count - q) % rows_count).wait_recv())
    own_fin.wait()
    for part in range(2):
        for t in range(tiles):
            out_ref[part, :, t * SIDE:(t + 1) * SIDE] = fin_in[t // 8, part, :, t % 8, :]

    for field in range(3):
        each_row_peer(lambda q: slab_copy(field, q, my_r).wait_send())
    each_row_peer(lambda q: fin_copy(q, my_r).wait_send())

    def row_left(row, carry):
        def spec_left(field, carry):
            each_peer(lambda q: spec_copy(field, row, q, my_block).wait_send())
            return carry

        lax.fori_loop(0, 3, spec_left, 0)
        for g in range(len(LEG_GROUPS)):
            each_peer(lambda q: legs_copy(row, g, q, me).wait_send())
        each_peer(lambda q: cur_copy(row, q, my_block).wait_send())
        each_peer(lambda q: est_copy(row, q, me).wait_send())
        return carry

    lax.fori_loop(0, local_rows, row_left, 0)


def long_tables(total_rows):
    index = np.arange(SIDE)
    angle = 2.0 * np.pi * (index[:, None] * index[None, :] % SIDE) / SIDE
    c, s = np.cos(angle), np.sin(angle)
    forward = np.block([[c, s], [-s, c]]).astype(np.float32)
    tables = np.stack([forward, forward.T])
    top = tables.astype(jnp.bfloat16)
    rest = (tables - top.astype(np.float32)).astype(jnp.bfloat16)
    turn = 2.0 * np.pi * (index[:, None] * index[None, :]) / NC
    scale = 1.0 / (NC * total_rows)
    twiddle = np.stack(
        [np.cos(turn), -np.sin(turn), scale * np.cos(turn), scale * np.sin(turn)]
    ).astype(np.float32)
    return np.stack([top, rest], axis=1), twiddle


def fused_body(rows_count, fields_count, sky_maps, band_cuts, filters, wiener, response):
    groups = rows_count * fields_count
    local_rows = response.shape[0]
    total_rows = local_rows * groups
    in_rows = total_rows // rows_count
    table, twiddle = long_tables(total_rows)
    weight = jnp.concatenate([filters, wiener, response[None]]).reshape(
        6, local_rows, SIDE, SIDE
    )
    vmem = pl.BlockSpec(memory_space=pltpu.VMEM)
    f32 = jnp.float32
    dma = pltpu.SemaphoreType.DMA
    slab = pltpu.VMEM((rows_count, 3, in_rows) + TILE, f32)
    chunk = pltpu.VMEM((local_rows, groups, 2) + TILE, f32)
    lines = pltpu.VMEM((local_rows, 2, groups) + TILE, f32)
    final = pltpu.VMEM((rows_count, 2, in_rows) + TILE, f32)
    return pl.pallas_call(
        functools.partial(lens_kernel, rows_count, fields_count, local_rows),
        out_shape=jax.ShapeDtypeStruct((2,) + sky_maps.shape[1:], f32),
        in_specs=[pl.BlockSpec(memory_space=pltpu.SMEM)] + [vmem] * 4,
        out_specs=vmem,
        scratch_shapes=[
            slab, slab,
            pltpu.VMEM((3, local_rows, groups, 2) + TILE, f32),
            pltpu.VMEM((3, local_rows, 2, groups) + TILE, f32),
            pltpu.VMEM((6, local_rows, SIDE, SIDE), f32),
            pltpu.VMEM((local_rows, 5, 2, groups) + TILE, f32),
            pltpu.VMEM((local_rows, groups, 5, 2) + TILE, f32),
            pltpu.VMEM((5, 2, total_rows) + TILE, f32),
            pltpu.VMEM((2, total_rows) + TILE, f32),
            chunk, lines, lines, chunk, final, final,
            dma((2, 3, rows_count)), dma((2, 3, local_rows, groups - 1)),
            dma((2, local_rows, len(LEG_GROUPS), groups - 1)),
            dma((2, local_rows, groups - 1)), dma((2, local_rows, groups - 1)),
            dma((2, rows_count)), dma((4 + (5 + len(LEG_GROUPS)) * local_rows,)),
        ],
        compiler_params=pltpu.CompilerParams(
            collective_id=0, has_side_effects=True, vmem_limit_bytes=48 * 1024 * 1024
        ),
        name="lens",
    )(band_cuts, sky_maps, weight, jnp.asarray(table), jnp.asarray(twiddle))


def solution(mesh):
    placed = (
        P("sims", "rows", "fields"),
        P(),
        P(None, ("rows", "fields"), None),
        P(None, ("rows", "fields"), None),
        P(("rows", "fields"), None),
    )
    rows_count, fields_count = mesh.shape["rows"], mesh.shape["fields"]
    groups = rows_count * fields_count

    def choose(sky_maps, *rest):
        fits = (
            NC == SIDE * SIDE
            and fields_count % 2 == 0
            and NC // groups == TILE[0] * TILE[1]
            and sky_maps.shape[1] % 8 == 0
            and sky_maps.shape[1] * rows_count in (16, 32, 64)
        )
        if fits:
            return fused_body(rows_count, fields_count, sky_maps, *rest)
        return body(sky_maps, *rest)

    return jax.shard_map(
        choose, mesh=mesh, in_specs=placed, out_specs=P("sims", "rows", "fields"), check_vma=False
    )
```

```python
import functools
import math

import jax
import jax.numpy as jnp
import numpy as np
from jax import lax
from jax.experimental import pallas as pl
from jax.experimental.pallas import tpu as pltpu
from jax.sharding import PartitionSpec as P

NC = 16384


exact_mode = lax.Precision.HIGHEST


def split_factor(length):
    best_first = 1
    for divisor in range(1, math.isqrt(length) + 1):
        if length % divisor == 0:
            best_first = divisor
    return (best_first, length // best_first)


def phase_table(left_index, right_index, period, direction):
    product = left_index[:, None] * right_index[None, :] % period
    angles = direction * 2.0 * math.pi / period * product.astype(jnp.float32)
    return (jnp.cos(angles), jnp.sin(angles))


def complex_einsum(formula, data_pair, table_pair):
    data_real, data_imag = data_pair
    table_real, table_imag = table_pair
    real_out = jnp.einsum(formula, data_real, table_real, precision=exact_mode)
    imag_out = jnp.einsum(formula, data_real, table_imag, precision=exact_mode)
    if data_imag is not None:
        real_out = real_out - jnp.einsum(formula, data_imag, table_imag, precision=exact_mode)
        imag_out = imag_out + jnp.einsum(formula, data_imag, table_real, precision=exact_mode)
    return (real_out, imag_out)


def complex_mul(left_pair, right_pair):
    return (
        left_pair[0] * right_pair[0] - left_pair[1] * right_pair[1],
        left_pair[0] * right_pair[1] + left_pair[1] * right_pair[0],
    )


def conj_mul(left_pair, right_pair):
    return (
        left_pair[0] * right_pair[0] + left_pair[1] * right_pair[1],
        left_pair[0] * right_pair[1] - left_pair[1] * right_pair[0],
    )


def row_transform(data_pair, direction):
    batch_len, length, block_width = data_pair[0].shape
    outer_len, inner_len = split_factor(length)
    outer_ids = jnp.arange(outer_len, dtype=jnp.int32)
    inner_ids = jnp.arange(inner_len, dtype=jnp.int32)
    real_in = data_pair[0].reshape(batch_len, outer_len, inner_len, block_width)
    imag_in = None
    if data_pair[1] is not None:
        imag_in = data_pair[1].reshape(batch_len, outer_len, inner_len, block_width)
    middle = complex_einsum(
        "bjmc,jk->bkmc", (real_in, imag_in), phase_table(outer_ids, outer_ids, outer_len, direction)
    )
    twiddle = phase_table(outer_ids, inner_ids, length, direction)
    middle = complex_mul(middle, (twiddle[0][None, :, :, None], twiddle[1][None, :, :, None]))
    result = complex_einsum(
        "bkmc,mq->bqkc", middle, phase_table(inner_ids, inner_ids, inner_len, direction)
    )
    norm_factor = 1.0 if direction < 0 else 1.0 / length
    return (
        result[0].reshape(batch_len, length, block_width) * norm_factor,
        result[1].reshape(batch_len, length, block_width) * norm_factor,
    )


def block_order(groups, fields_count):
    positions = jnp.arange(groups, dtype=jnp.int32)
    blocks = positions % fields_count * (groups // fields_count) + positions // fields_count
    return (positions, blocks)


def column_forward(data_pair, groups, fields_count):
    batch_len, local_rows, total_len = data_pair[0].shape
    block_width = total_len // groups
    positions, blocks = block_order(groups, fields_count)
    column_ids = jnp.arange(block_width, dtype=jnp.int32)
    shaped = (
        data_pair[0].reshape(batch_len, local_rows, groups, block_width),
        data_pair[1].reshape(batch_len, local_rows, groups, block_width),
    )
    middle = complex_einsum("brpc,pk->brkc", shaped, phase_table(blocks, positions, groups, -1.0))
    twiddle = phase_table(positions, column_ids, total_len, -1.0)
    middle = complex_mul(middle, (twiddle[0][None, None], twiddle[1][None, None]))
    result = complex_einsum(
        "brkc,cq->brqk", middle, phase_table(column_ids, column_ids, block_width, -1.0)
    )
    return (
        result[0].reshape(batch_len, local_rows, total_len),
        result[1].reshape(batch_len, local_rows, total_len),
    )


def column_inverse(data_pair, groups, fields_count):
    batch_len, local_rows, total_len = data_pair[0].shape
    block_width = total_len // groups
    positions, blocks = block_order(groups, fields_count)
    column_ids = jnp.arange(block_width, dtype=jnp.int32)
    shaped = (
        data_pair[0].reshape(batch_len, local_rows, block_width, groups),
        data_pair[1].reshape(batch_len, local_rows, block_width, groups),
    )
    middle = complex_einsum(
        "brqk,qc->brkc", shaped, phase_table(column_ids, column_ids, block_width, 1.0)
    )
    twiddle = phase_table(positions, column_ids, total_len, 1.0)
    middle = complex_mul(middle, (twiddle[0][None, None], twiddle[1][None, None]))
    result = complex_einsum("brkc,kp->brpc", middle, phase_table(positions, blocks, groups, 1.0))
    norm_factor = 1.0 / total_len
    return (
        result[0].reshape(batch_len, local_rows, total_len) * norm_factor,
        result[1].reshape(batch_len, local_rows, total_len) * norm_factor,
    )


def body(sky_maps, band_cuts, filters, wiener, response):
    rows_count = lax.axis_size("rows")
    fields_count = lax.axis_size("fields")
    groups = rows_count * fields_count
    local_rows = filters.shape[1]
    total_rows = local_rows * groups
    row_ratio = NC // total_rows

    def forward_columns(stacked):
        return jnp.stack(column_forward((stacked[0], stacked[1]), groups, fields_count))

    def inverse_rows(stacked):
        return jnp.stack(row_transform((stacked[0], stacked[1]), 1.0))

    def inverse_columns(stacked):
        return jnp.stack(column_inverse((stacked[0], stacked[1]), groups, fields_count))

    def to_frequency(stacked):
        batch_len = stacked.shape[1]
        block_width = stacked.shape[3]
        shaped = stacked.reshape(
            2, batch_len, rows_count, fields_count, local_rows, 1, 1, block_width
        )
        arrived = lax.all_to_all(
            lax.all_to_all(shaped, "rows", split_axis=2, concat_axis=5, tiled=True),
            "fields",
            split_axis=3,
            concat_axis=6,
            tiled=True,
        )
        result = forward_columns(arrived.reshape(2, batch_len, local_rows, groups * block_width))
        return result

    def to_space(stacked):
        batch_len = stacked.shape[1]
        block_width = stacked.shape[3] // groups
        shaped = stacked.reshape(
            2, batch_len, 1, 1, local_rows, rows_count, fields_count, block_width
        )
        arrived = lax.all_to_all(
            lax.all_to_all(shaped, "rows", split_axis=5, concat_axis=2, tiled=True),
            "fields",
            split_axis=6,
            concat_axis=3,
            tiled=True,
        )
        result = inverse_rows(arrived.reshape(2, batch_len, total_rows, block_width))
        return result

    slab_spectra = jnp.stack(
        row_transform(
            (lax.all_to_all(sky_maps, "rows", split_axis=2, concat_axis=1, tiled=True), None), -1.0
        )
    )
    sky_spectra = to_frequency(slab_spectra)
    row_ids = lax.axis_index(("rows", "fields")) * local_rows + jnp.arange(
        local_rows, dtype=jnp.int32
    )
    freq_rows = jnp.where(row_ids < total_rows // 2, row_ids, row_ids - total_rows)[:, None]
    column_ids = jnp.arange(NC, dtype=jnp.int32)
    freq_cols = jnp.where(column_ids < NC // 2, column_ids, column_ids - NC)[None, :]
    scaled_rows = row_ratio * freq_rows
    radius_sq = freq_cols * freq_cols + scaled_rows * scaled_rows

    def band_mask(lower_cut, upper_cut):
        inside = (radius_sq >= lower_cut * lower_cut) & (radius_sq <= upper_cut * upper_cut)
        return inside.astype(jnp.float32)

    mask_temp = band_mask(band_cuts[0], band_cuts[1])
    mask_pol = band_mask(band_cuts[2], band_cuts[3])
    mask_out = band_mask(band_cuts[4], band_cuts[5])
    radius_floor = jnp.maximum(radius_sq, 1).astype(jnp.float32)
    cos_two = (freq_cols * freq_cols - scaled_rows * scaled_rows).astype(jnp.float32) / radius_floor
    sin_two = (2 * freq_cols * scaled_rows).astype(jnp.float32) / radius_floor
    along_x = (2 * freq_cols).astype(jnp.float32) / NC
    along_y = (2 * freq_rows).astype(jnp.float32) / total_rows
    raising = (-along_y + 0.0 * along_x, along_x + 0.0 * along_y)
    lowering = (along_y + 0.0 * along_x, along_x + 0.0 * along_y)
    rotation = (cos_two, sin_two)
    temp_modes = (sky_spectra[0, 0], sky_spectra[1, 0])
    stokes_q = (sky_spectra[0, 1], sky_spectra[1, 1])
    stokes_u = (sky_spectra[0, 2], sky_spectra[1, 2])
    e_modes = (
        -(cos_two * stokes_q[0] + sin_two * stokes_u[0]),
        -(cos_two * stokes_q[1] + sin_two * stokes_u[1]),
    )
    b_modes = (
        sin_two * stokes_q[0] - cos_two * stokes_u[0],
        sin_two * stokes_q[1] - cos_two * stokes_u[1],
    )
    temp_weight = mask_temp * filters[0]
    e_weight = mask_pol * filters[1]
    b_weight = mask_pol * filters[2]
    temp_bar = (temp_weight * temp_modes[0], temp_weight * temp_modes[1])
    e_bar = (e_weight * e_modes[0], e_weight * e_modes[1])
    b_bar = (b_weight * b_modes[0], b_weight * b_modes[1])
    grad_temp = complex_mul(raising, (wiener[0] * temp_bar[0], wiener[0] * temp_bar[1]))
    pol_sum = complex_mul((e_bar[0] - b_bar[1], e_bar[1] + b_bar[0]), rotation)
    pol_bar = (-pol_sum[0], -pol_sum[1])
    pol_rot = complex_mul((wiener[1] * e_bar[0], wiener[1] * e_bar[1]), rotation)
    pol_wiener = (-pol_rot[0], -pol_rot[1])
    spin_three = complex_mul(raising, pol_wiener)
    spin_one = complex_mul(lowering, pol_wiener)
    leg_spectra = jnp.stack(
        [
            jnp.stack([temp_bar[0], grad_temp[0], pol_bar[0], spin_three[0], spin_one[0]]),
            jnp.stack([temp_bar[1], grad_temp[1], pol_bar[1], spin_three[1], spin_one[1]]),
        ]
    )
    leg_maps = to_space(inverse_columns(leg_spectra))
    temp_leg = (leg_maps[0, 0], leg_maps[1, 0])
    grad_leg = (leg_maps[0, 1], leg_maps[1, 1])
    pol_leg = (leg_maps[0, 2], leg_maps[1, 2])
    three_leg = (leg_maps[0, 3], leg_maps[1, 3])
    one_leg = (leg_maps[0, 4], leg_maps[1, 4])
    temp_term = complex_mul(temp_leg, grad_leg)
    raise_term = conj_mul(pol_leg, three_leg)
    lower_term = conj_mul(one_leg, pol_leg)
    current = (
        temp_term[0] + 0.5 * (raise_term[0] + lower_term[0]),
        temp_term[1] + 0.5 * (raise_term[1] + lower_term[1]),
    )
    current_rows = jnp.stack(row_transform((current[0][None], current[1][None]), -1.0))
    current_modes = to_frequency(current_rows)
    out_weight = mask_out * response
    estimate_modes = complex_mul(
        lowering, (out_weight * current_modes[0, 0], out_weight * current_modes[1, 0])
    )
    estimate_stack = jnp.stack([estimate_modes[0][None], estimate_modes[1][None]])
    estimate_maps = to_space(inverse_columns(estimate_stack))
    slab_result = estimate_maps[:, 0]
    return lax.all_to_all(slab_result, "rows", split_axis=1, concat_axis=2, tiled=True)


SIDE = 128
TILE = (8, 128)
LEG_GROUPS = ((0, 2), (2, 2), (4, 1))
MESH = pl.DeviceIdType.MESH


def add_pair(a, b):
    imag = a[1] if b[1] is None else b[1] if a[1] is None else a[1] + b[1]
    return (a[0] + b[0], imag)


def sub_pair(a, b):
    imag = a[1] if b[1] is None else -b[1] if a[1] is None else a[1] - b[1]
    return (a[0] - b[0], imag)


def turn_pair(value, step, length, direction):
    real, imag = value
    if step == 0:
        return value
    if 4 * step == length:
        if imag is None:
            return (jnp.zeros_like(real), real if direction > 0 else -real)
        return (-imag, real) if direction > 0 else (imag, -real)
    angle = 2.0 * math.pi * step / length
    c, s = math.cos(angle), direction * math.sin(angle)
    if imag is None:
        return (real * c, real * s)
    if 8 * step == length:
        if direction > 0:
            return ((real - imag) * c, (real + imag) * c)
        return ((real + imag) * c, (imag - real) * c)
    if 8 * step == 3 * length:
        if direction > 0:
            return ((real + imag) * c, (imag - real) * c)
        return ((real - imag) * c, (real + imag) * c)
    return (real * c - imag * s, real * s + imag * c)


def short_transform(values, direction):
    length = len(values)
    if length == 1:
        return values
    even = short_transform(values[0::2], direction)
    odd = short_transform(values[1::2], direction)
    low, high = [], []
    for step in range(length // 2):
        turned = turn_pair(odd[step], step, length, direction)
        low.append(add_pair(even[step], turned))
        high.append(sub_pair(even[step], turned))
    return low + high


def split_number(x):
    top = x.astype(jnp.bfloat16)
    return top, (x - top.astype(jnp.float32)).astype(jnp.bfloat16)


def dot32(a, b):
    return jnp.dot(a, b, preferred_element_type=jnp.float32)


def matrix_left(table_ref, which, x):
    top, rest = split_number(x)
    m_top, m_rest = table_ref[which, 0], table_ref[which, 1]
    return dot32(m_top, top) + (dot32(m_top, rest) + dot32(m_rest, top))


def matrix_right(table_ref, which, x):
    top, rest = split_number(x)
    m_top, m_rest = table_ref[which, 0], table_ref[which, 1]
    return dot32(top, m_top) + (dot32(top, m_rest) + dot32(rest, m_top))


def lens_kernel(
    rows_count, fields_count, local_rows,
    cuts_ref, sky_ref, weight_ref, table_ref, twiddle_ref, out_ref,
    slab_out, slab_in, spec_out, spec_in, weights, legs_out, legs_in, maps, current,
    cur_out, cur_in, est_out, est_in, fin_out, fin_in,
    slab_sem, spec_sem, legs_sem, cur_sem, est_sem, fin_sem, self_sem,
):
    groups = rows_count * fields_count
    total_rows = groups * local_rows
    in_rows = total_rows // rows_count
    row_ratio = NC // total_rows
    my_r, my_f = lax.axis_index("rows"), lax.axis_index("fields")
    me = my_r * fields_count + my_f
    my_block = my_f * rows_count + my_r

    half = fields_count // 2
    my_half, my_spot = my_f // half, my_f % half

    def wrapped(value, length):
        return jnp.where(value >= length, value - length, value)

    row_at = [wrapped(my_r + d, rows_count) for d in range(rows_count)]
    spot_at = [wrapped(my_spot + d, half) for d in range(half)]
    side_at = [my_half * half, (1 - my_half) * half]

    def partner(q, sign):
        side = 1 - q // (rows_count * half)
        spot = sign * (q // rows_count + 1) % half
        return row_at[sign * (q + 1) % rows_count], side_at[side] + spot_at[spot]

    def peer_of(q):
        r, f = partner(q, 1)
        return r * fields_count + f

    def source_of(q):
        r, f = partner(q, -1)
        return r * fields_count + f

    def peer_block(q):
        r, f = partner(q, 1)
        return f * rows_count + r

    def source_block(q):
        r, f = partner(q, -1)
        return f * rows_count + r

    def target(q):
        r, f = partner(q, 1)
        return {"rows": r, "fields": f}

    def send(q, src, dst, sems):
        return pltpu.make_async_remote_copy(
            src_ref=src, dst_ref=dst, send_sem=sems[0], recv_sem=sems[1],
            device_id=target(q), device_id_type=MESH,
        )

    def send_row(q, src, dst, sems):
        return pltpu.make_async_remote_copy(
            src_ref=src, dst_ref=dst, send_sem=sems[0], recv_sem=sems[1],
            device_id={"rows": row_at[q]}, device_id_type=MESH,
        )

    def each_peer(body):
        for q in range(groups - 1):
            body(q)

    def each_row_peer(body):
        for q in range(1, rows_count):
            body(q)

    barrier = pltpu.get_barrier_semaphore()

    def greet(q):
        pl.semaphore_signal(
            barrier, inc=1, device_id=target(q), device_id_type=MESH
        )

    each_peer(greet)
    tiles = sky_ref.shape[2] // SIDE
    for field in range(3):
        for t in range(tiles):
            slab_out[t // 8, field, :, t % 8, :] = sky_ref[field, :, t * SIDE:(t + 1) * SIDE]
    pl.semaphore_wait(barrier, groups - 1)

    def slab_copy(field, q, src_row):
        return send_row(
            q, slab_out.at[row_at[q], field], slab_in.at[src_row, field],
            (slab_sem.at[0, field, q], slab_sem.at[1, field, q]),
        )

    def own_slab(field):
        return pltpu.make_async_copy(
            slab_out.at[my_r, field], slab_in.at[my_r, field], self_sem.at[field]
        )

    for field in range(3):
        each_row_peer(lambda q: slab_copy(field, q, my_r).start())
        own_slab(field).start()

    low_index = lax.broadcasted_iota(jnp.int32, (SIDE, SIDE), 0)
    high_index = lax.broadcasted_iota(jnp.int32, (SIDE, SIDE), 1)
    column_ids = low_index + SIDE * high_index
    freq_cols = jnp.where(column_ids < NC // 2, column_ids, column_ids - NC)

    def row_frequency(row):
        row_id = me * local_rows + row
        return jnp.where(row_id < total_rows // 2, row_id, row_id - total_rows)

    def weigh(row, carry):
        scaled = row_ratio * row_frequency(row)
        radius_sq = freq_cols * freq_cols + scaled * scaled

        def mask(n):
            low, high = cuts_ref[2 * n], cuts_ref[2 * n + 1]
            inside = (radius_sq >= low * low) & (radius_sq <= high * high)
            return inside.astype(jnp.float32)

        pol = mask(1)
        weights[0, row] = mask(0) * weight_ref[0, row].T
        weights[1, row] = pol * weight_ref[1, row].T
        weights[2, row] = pol * weight_ref[2, row].T
        weights[3, row] = weight_ref[3, row].T
        weights[4, row] = weight_ref[4, row].T
        weights[5, row] = mask(2) * weight_ref[5, row].T
        return carry

    lax.fori_loop(0, local_rows, weigh, 0)

    def spec_copy(field, row, q, src_block):
        return send(
            q, spec_out.at[field, row, peer_of(q)], spec_in.at[field, row, :, src_block],
            (spec_sem.at[0, field, row, q], spec_sem.at[1, field, row, q]),
        )

    def own_spec(field, row):
        return pltpu.make_async_copy(
            spec_out.at[field, row, me], spec_in.at[field, row, :, my_block],
            self_sem.at[3 + field * local_rows + row],
        )

    def spec_start(field, row):
        each_peer(lambda q: spec_copy(field, row, q, my_block).start())
        own_spec(field, row).start()

    def row_step(field, carry):
        each_row_peer(
            lambda q: slab_copy(field, q, row_at[rows_count - q]).wait_recv()
        )
        own_slab(field).wait()
        values = [
            (slab_in[y // in_rows, field, y % in_rows], None) for y in range(total_rows)
        ]
        for k, (real, imag) in enumerate(short_transform(values, -1)):
            spec_out[field, k % local_rows, k // local_rows, 0] = real
            spec_out[field, k % local_rows, k // local_rows, 1] = (
                jnp.zeros_like(real) if imag is None else imag
            )
        spec_start(field, 0)
        return carry

    lax.fori_loop(0, 3, row_step, 0)

    def later_rows(n, carry):
        spec_start(n % 3, 1 + n // 3)
        return carry

    lax.fori_loop(0, 3 * (local_rows - 1), later_rows, 0)

    def spec_wait(row):
        def step(field, carry):
            each_peer(lambda q: spec_copy(field, row, q, source_block(q)).wait_recv())
            own_spec(field, row).wait()
            return carry

        lax.fori_loop(0, 3, step, 0)

    cos_f, sin_f, cos_b, sin_b = 0, 1, 2, 3

    def side_by_side(pieces, axis):
        return pieces[0] if len(pieces) == 1 else jnp.concatenate(pieces, axis=axis)

    def long_forward(pieces):
        y = matrix_left(table_ref, 0, side_by_side(pieces, 1))
        c, s = twiddle_ref[cos_f], twiddle_ref[sin_f]
        turned = []
        for n in range(len(pieces)):
            yr, yi = y[:SIDE, n * SIDE:(n + 1) * SIDE], y[SIDE:, n * SIDE:(n + 1) * SIDE]
            turned.append(jnp.concatenate([yr * c - yi * s, yr * s + yi * c], axis=1))
        z = matrix_right(table_ref, 1, side_by_side(turned, 0))
        return [
            (z[n * SIDE:(n + 1) * SIDE, :SIDE], z[n * SIDE:(n + 1) * SIDE, SIDE:])
            for n in range(len(pieces))
        ]

    def long_inverse(pairs):
        stacks = [jnp.concatenate([pair[0], pair[1]], axis=1) for pair in pairs]
        u = matrix_right(table_ref, 0, side_by_side(stacks, 0))
        c, s = twiddle_ref[cos_b], twiddle_ref[sin_b]
        turned = []
        for n in range(len(pairs)):
            ur, ui = u[n * SIDE:(n + 1) * SIDE, :SIDE], u[n * SIDE:(n + 1) * SIDE, SIDE:]
            turned.append(jnp.concatenate([ur * c - ui * s, ur * s + ui * c], axis=0))
        x = matrix_left(table_ref, 1, side_by_side(turned, 1))
        return [
            x[:, n * SIDE:(n + 1) * SIDE].reshape((2, groups) + TILE)
            for n in range(len(pairs))
        ]

    leg_self = 3 + 3 * local_rows

    def legs_copy(row, g, q, src_index):
        first, count = LEG_GROUPS[g]
        return send(
            q, legs_out.at[row, first:first + count, :, peer_block(q)],
            legs_in.at[row, src_index, first:first + count],
            (legs_sem.at[0, row, g, q], legs_sem.at[1, row, g, q]),
        )

    def own_legs(row, g):
        first, count = LEG_GROUPS[g]
        return pltpu.make_async_copy(
            legs_out.at[row, first:first + count, :, my_block],
            legs_in.at[row, me, first:first + count],
            self_sem.at[leg_self + row * len(LEG_GROUPS) + g],
        )

    def slopes(row):
        along_x = (2 * freq_cols).astype(jnp.float32) / NC
        along_y = (2 * row_frequency(row)).astype(jnp.float32) / total_rows
        return along_x, along_y

    def leg_step(row, carry):
        spec_wait(row)
        temp, stokes_q, stokes_u = long_forward(
            [spec_in[field, row].reshape(2 * SIDE, SIDE) for field in range(3)]
        )
        scaled = row_ratio * row_frequency(row)
        radius_sq = freq_cols * freq_cols + scaled * scaled
        floor = jnp.maximum(radius_sq, 1).astype(jnp.float32)
        cos2 = (freq_cols * freq_cols - scaled * scaled).astype(jnp.float32) / floor
        sin2 = (2 * freq_cols * scaled).astype(jnp.float32) / floor
        along_x, along_y = slopes(row)
        raising, lowering = (-along_y, along_x), (along_y, along_x)
        rot = (cos2, sin2)
        w_t, w_e, w_b = weights[0, row], weights[1, row], weights[2, row]
        w_gt, w_ge = weights[3, row], weights[4, row]
        t_bar = (w_t * temp[0], w_t * temp[1])
        e_bar = tuple(-w_e * (cos2 * a + sin2 * b) for a, b in zip(stokes_q, stokes_u))
        b_bar = tuple(w_b * (sin2 * a - cos2 * b) for a, b in zip(stokes_q, stokes_u))
        g = complex_mul((w_gt * t_bar[0], w_gt * t_bar[1]), raising)
        p = complex_mul((b_bar[1] - e_bar[0], -(e_bar[1] + b_bar[0])), rot)
        w = complex_mul((-w_ge * e_bar[0], -w_ge * e_bar[1]), rot)
        h3 = complex_mul(w, raising)
        h1 = complex_mul(w, lowering)
        legs = (t_bar, g, p, h3, h1)
        for n, (first, count) in enumerate(LEG_GROUPS):
            for k, leg_map in enumerate(long_inverse(legs[first:first + count])):
                legs_out[row, first + k] = leg_map
            each_peer(lambda q: legs_copy(row, n, q, me).start())
            own_legs(row, n).start()
        return carry

    lax.fori_loop(0, local_rows, leg_step, 0)

    for field in range(3):
        each_row_peer(lambda q: slab_copy(field, q, my_r).wait_send())

    def spec_left(n, carry):
        each_peer(lambda q: spec_copy(n % 3, n // 3, q, my_block).wait_send())
        return carry

    lax.fori_loop(0, 3 * local_rows, spec_left, 0)

    def leg_wait(g):
        def step(row, carry):
            each_peer(lambda q: legs_copy(row, g, q, source_of(q)).wait_recv())
            own_legs(row, g).wait()
            return carry

        lax.fori_loop(0, local_rows, step, 0)

    def map_step(n, carry):
        values = [
            (legs_in[k % local_rows, k // local_rows, n, 0],
             legs_in[k % local_rows, k // local_rows, n, 1])
            for k in range(total_rows)
        ]
        for y, (real, imag) in enumerate(short_transform(values, 1)):
            maps[n, 0, y] = real
            maps[n, 1, y] = imag
        return carry

    for g, (first, count) in enumerate(LEG_GROUPS):
        leg_wait(g)
        lax.fori_loop(first, first + count, map_step, 0)

    def product_step(y, carry):
        a, g, p, h3, h1 = [(maps[n, 0, y], maps[n, 1, y]) for n in range(5)]
        ag, ph, hp = complex_mul(a, g), conj_mul(p, h3), conj_mul(h1, p)
        current[0, y] = ag[0] + 0.5 * (ph[0] + hp[0])
        current[1, y] = ag[1] + 0.5 * (ph[1] + hp[1])
        return carry

    lax.fori_loop(0, total_rows, product_step, 0)

    values = [(current[0, y], current[1, y]) for y in range(total_rows)]
    for k, (real, imag) in enumerate(short_transform(values, -1)):
        cur_out[k % local_rows, k // local_rows, 0] = real
        cur_out[k % local_rows, k // local_rows, 1] = imag
    cur_self = leg_self + len(LEG_GROUPS) * local_rows
    est_self = cur_self + local_rows

    def cur_copy(row, q, src_block):
        return send(
            q, cur_out.at[row, peer_of(q)], cur_in.at[row, :, src_block],
            (cur_sem.at[0, row, q], cur_sem.at[1, row, q]),
        )

    def own_cur(row):
        return pltpu.make_async_copy(
            cur_out.at[row, me], cur_in.at[row, :, my_block], self_sem.at[cur_self + row]
        )

    def cur_start(row, carry):
        each_peer(lambda q: cur_copy(row, q, my_block).start())
        own_cur(row).start()
        return carry

    lax.fori_loop(0, local_rows, cur_start, 0)

    def legs_left(row, carry):
        for g in range(len(LEG_GROUPS)):
            each_peer(lambda q: legs_copy(row, g, q, me).wait_send())
        return carry

    lax.fori_loop(0, local_rows, legs_left, 0)

    def est_copy(row, q, src_index):
        return send(
            q, est_out.at[row, :, peer_block(q)], est_in.at[row, src_index],
            (est_sem.at[0, row, q], est_sem.at[1, row, q]),
        )

    def own_est(row):
        return pltpu.make_async_copy(
            est_out.at[row, :, my_block], est_in.at[row, me], self_sem.at[est_self + row]
        )

    def estimate_step(row, carry):
        each_peer(lambda q: cur_copy(row, q, source_block(q)).wait_recv())
        own_cur(row).wait()
        (modes,) = long_forward([cur_in[row].reshape(2 * SIDE, SIDE)])
        along_x, along_y = slopes(row)
        w = weights[5, row]
        estimate = complex_mul((w * modes[0], w * modes[1]), (along_y, along_x))
        (est_out[row],) = long_inverse([estimate])
        each_peer(lambda q: est_copy(row, q, me).start())
        own_est(row).start()
        return carry

    lax.fori_loop(0, local_rows, estimate_step, 0)

    def cur_left(row, carry):
        each_peer(lambda q: cur_copy(row, q, my_block).wait_send())
        return carry

    lax.fori_loop(0, local_rows, cur_left, 0)

    def est_wait(row, carry):
        each_peer(lambda q: est_copy(row, q, source_of(q)).wait_recv())
        own_est(row).wait()
        return carry

    lax.fori_loop(0, local_rows, est_wait, 0)

    values = [
        (est_in[k % local_rows, k // local_rows, 0], est_in[k % local_rows, k // local_rows, 1])
        for k in range(total_rows)
    ]
    for y, (real, imag) in enumerate(short_transform(values, 1)):
        fin_out[y // in_rows, 0, y % in_rows] = real
        fin_out[y // in_rows, 1, y % in_rows] = imag

    def fin_copy(q, src_row):
        return send_row(
            q, fin_out.at[row_at[q]], fin_in.at[src_row],
            (fin_sem.at[0, q], fin_sem.at[1, q]),
        )

    each_row_peer(lambda q: fin_copy(q, my_r).start())
    own_fin = pltpu.make_async_copy(
        fin_out.at[my_r], fin_in.at[my_r], self_sem.at[est_self + local_rows]
    )
    own_fin.start()

    def est_left(row, carry):
        each_peer(lambda q: est_copy(row, q, me).wait_send())
        return carry

    lax.fori_loop(0, local_rows, est_left, 0)
    each_row_peer(lambda q: fin_copy(q, row_at[rows_count - q]).wait_recv())
    own_fin.wait()
    for part in range(2):
        for t in range(tiles):
            out_ref[part, :, t * SIDE:(t + 1) * SIDE] = fin_in[t // 8, part, :, t % 8, :]

    each_row_peer(lambda q: fin_copy(q, my_r).wait_send())


def long_tables(total_rows):
    index = np.arange(SIDE)
    angle = 2.0 * np.pi * (index[:, None] * index[None, :] % SIDE) / SIDE
    c, s = np.cos(angle), np.sin(angle)
    forward = np.block([[c, s], [-s, c]]).astype(np.float32)
    tables = np.stack([forward, forward.T])
    top = tables.astype(jnp.bfloat16)
    rest = (tables - top.astype(np.float32)).astype(jnp.bfloat16)
    turn = 2.0 * np.pi * (index[:, None] * index[None, :]) / NC
    scale = 1.0 / (NC * total_rows)
    twiddle = np.stack(
        [np.cos(turn), -np.sin(turn), scale * np.cos(turn), scale * np.sin(turn)]
    ).astype(np.float32)
    return np.stack([top, rest], axis=1), twiddle


def fused_body(rows_count, fields_count, sky_maps, band_cuts, filters, wiener, response):
    groups = rows_count * fields_count
    local_rows = response.shape[0]
    total_rows = local_rows * groups
    in_rows = total_rows // rows_count
    table, twiddle = long_tables(total_rows)
    weight = jnp.concatenate([filters, wiener, response[None]]).reshape(
        6, local_rows, SIDE, SIDE
    )
    vmem = pl.BlockSpec(memory_space=pltpu.VMEM)
    f32 = jnp.float32
    dma = pltpu.SemaphoreType.DMA
    slab = pltpu.VMEM((rows_count, 3, in_rows) + TILE, f32)
    chunk = pltpu.VMEM((local_rows, groups, 2) + TILE, f32)
    lines = pltpu.VMEM((local_rows, 2, groups) + TILE, f32)
    final = pltpu.VMEM((rows_count, 2, in_rows) + TILE, f32)
    return pl.pallas_call(
        functools.partial(lens_kernel, rows_count, fields_count, local_rows),
        out_shape=jax.ShapeDtypeStruct((2,) + sky_maps.shape[1:], f32),
        in_specs=[pl.BlockSpec(memory_space=pltpu.SMEM)] + [vmem] * 4,
        out_specs=vmem,
        scratch_shapes=[
            slab, slab,
            pltpu.VMEM((3, local_rows, groups, 2) + TILE, f32),
            pltpu.VMEM((3, local_rows, 2, groups) + TILE, f32),
            pltpu.VMEM((6, local_rows, SIDE, SIDE), f32),
            pltpu.VMEM((local_rows, 5, 2, groups) + TILE, f32),
            pltpu.VMEM((local_rows, groups, 5, 2) + TILE, f32),
            pltpu.VMEM((5, 2, total_rows) + TILE, f32),
            pltpu.VMEM((2, total_rows) + TILE, f32),
            chunk, lines, lines, chunk, final, final,
            dma((2, 3, rows_count)), dma((2, 3, local_rows, groups - 1)),
            dma((2, local_rows, len(LEG_GROUPS), groups - 1)),
            dma((2, local_rows, groups - 1)), dma((2, local_rows, groups - 1)),
            dma((2, rows_count)), dma((4 + (5 + len(LEG_GROUPS)) * local_rows,)),
        ],
        compiler_params=pltpu.CompilerParams(
            collective_id=0, has_side_effects=True, vmem_limit_bytes=48 * 1024 * 1024
        ),
        name="lens",
    )(band_cuts, sky_maps, weight, jnp.asarray(table), jnp.asarray(twiddle))


def solution(mesh):
    placed = (
        P("sims", "rows", "fields"),
        P(),
        P(None, ("rows", "fields"), None),
        P(None, ("rows", "fields"), None),
        P(("rows", "fields"), None),
    )
    rows_count, fields_count = mesh.shape["rows"], mesh.shape["fields"]
    groups = rows_count * fields_count

    def choose(sky_maps, *rest):
        fits = (
            NC == SIDE * SIDE
            and fields_count % 2 == 0
            and NC // groups == TILE[0] * TILE[1]
            and sky_maps.shape[1] % 8 == 0
            and sky_maps.shape[1] * rows_count in (16, 32, 64)
        )
        if fits:
            return fused_body(rows_count, fields_count, sky_maps, *rest)
        return body(sky_maps, *rest)

    return jax.shard_map(
        choose, mesh=mesh, in_specs=placed, out_specs=P("sims", "rows", "fields"), check_vma=False
    )
```

```python
import functools
import math

import jax
import jax.numpy as jnp
import numpy as np
from jax import lax
from jax.experimental import pallas as pl
from jax.experimental.pallas import tpu as pltpu
from jax.sharding import PartitionSpec as P

NC = 16384


exact_mode = lax.Precision.HIGHEST


def split_factor(length):
    best_first = 1
    for divisor in range(1, math.isqrt(length) + 1):
        if length % divisor == 0:
            best_first = divisor
    return (best_first, length // best_first)


def phase_table(left_index, right_index, period, direction):
    product = left_index[:, None] * right_index[None, :] % period
    angles = direction * 2.0 * math.pi / period * product.astype(jnp.float32)
    return (jnp.cos(angles), jnp.sin(angles))


def complex_einsum(formula, data_pair, table_pair):
    data_real, data_imag = data_pair
    table_real, table_imag = table_pair
    real_out = jnp.einsum(formula, data_real, table_real, precision=exact_mode)
    imag_out = jnp.einsum(formula, data_real, table_imag, precision=exact_mode)
    if data_imag is not None:
        real_out = real_out - jnp.einsum(formula, data_imag, table_imag, precision=exact_mode)
        imag_out = imag_out + jnp.einsum(formula, data_imag, table_real, precision=exact_mode)
    return (real_out, imag_out)


def complex_mul(left_pair, right_pair):
    return (
        left_pair[0] * right_pair[0] - left_pair[1] * right_pair[1],
        left_pair[0] * right_pair[1] + left_pair[1] * right_pair[0],
    )


def conj_mul(left_pair, right_pair):
    return (
        left_pair[0] * right_pair[0] + left_pair[1] * right_pair[1],
        left_pair[0] * right_pair[1] - left_pair[1] * right_pair[0],
    )


def row_transform(data_pair, direction):
    batch_len, length, block_width = data_pair[0].shape
    outer_len, inner_len = split_factor(length)
    outer_ids = jnp.arange(outer_len, dtype=jnp.int32)
    inner_ids = jnp.arange(inner_len, dtype=jnp.int32)
    real_in = data_pair[0].reshape(batch_len, outer_len, inner_len, block_width)
    imag_in = None
    if data_pair[1] is not None:
        imag_in = data_pair[1].reshape(batch_len, outer_len, inner_len, block_width)
    middle = complex_einsum(
        "bjmc,jk->bkmc", (real_in, imag_in), phase_table(outer_ids, outer_ids, outer_len, direction)
    )
    twiddle = phase_table(outer_ids, inner_ids, length, direction)
    middle = complex_mul(middle, (twiddle[0][None, :, :, None], twiddle[1][None, :, :, None]))
    result = complex_einsum(
        "bkmc,mq->bqkc", middle, phase_table(inner_ids, inner_ids, inner_len, direction)
    )
    norm_factor = 1.0 if direction < 0 else 1.0 / length
    return (
        result[0].reshape(batch_len, length, block_width) * norm_factor,
        result[1].reshape(batch_len, length, block_width) * norm_factor,
    )


def block_order(groups, fields_count):
    positions = jnp.arange(groups, dtype=jnp.int32)
    blocks = positions % fields_count * (groups // fields_count) + positions // fields_count
    return (positions, blocks)


def column_forward(data_pair, groups, fields_count):
    batch_len, local_rows, total_len = data_pair[0].shape
    block_width = total_len // groups
    positions, blocks = block_order(groups, fields_count)
    column_ids = jnp.arange(block_width, dtype=jnp.int32)
    shaped = (
        data_pair[0].reshape(batch_len, local_rows, groups, block_width),
        data_pair[1].reshape(batch_len, local_rows, groups, block_width),
    )
    middle = complex_einsum("brpc,pk->brkc", shaped, phase_table(blocks, positions, groups, -1.0))
    twiddle = phase_table(positions, column_ids, total_len, -1.0)
    middle = complex_mul(middle, (twiddle[0][None, None], twiddle[1][None, None]))
    result = complex_einsum(
        "brkc,cq->brqk", middle, phase_table(column_ids, column_ids, block_width, -1.0)
    )
    return (
        result[0].reshape(batch_len, local_rows, total_len),
        result[1].reshape(batch_len, local_rows, total_len),
    )


def column_inverse(data_pair, groups, fields_count):
    batch_len, local_rows, total_len = data_pair[0].shape
    block_width = total_len // groups
    positions, blocks = block_order(groups, fields_count)
    column_ids = jnp.arange(block_width, dtype=jnp.int32)
    shaped = (
        data_pair[0].reshape(batch_len, local_rows, block_width, groups),
        data_pair[1].reshape(batch_len, local_rows, block_width, groups),
    )
    middle = complex_einsum(
        "brqk,qc->brkc", shaped, phase_table(column_ids, column_ids, block_width, 1.0)
    )
    twiddle = phase_table(positions, column_ids, total_len, 1.0)
    middle = complex_mul(middle, (twiddle[0][None, None], twiddle[1][None, None]))
    result = complex_einsum("brkc,kp->brpc", middle, phase_table(positions, blocks, groups, 1.0))
    norm_factor = 1.0 / total_len
    return (
        result[0].reshape(batch_len, local_rows, total_len) * norm_factor,
        result[1].reshape(batch_len, local_rows, total_len) * norm_factor,
    )


def body(sky_maps, band_cuts, filters, wiener, response):
    rows_count = lax.axis_size("rows")
    fields_count = lax.axis_size("fields")
    groups = rows_count * fields_count
    local_rows = filters.shape[1]
    total_rows = local_rows * groups
    row_ratio = NC // total_rows

    def forward_columns(stacked):
        return jnp.stack(column_forward((stacked[0], stacked[1]), groups, fields_count))

    def inverse_rows(stacked):
        return jnp.stack(row_transform((stacked[0], stacked[1]), 1.0))

    def inverse_columns(stacked):
        return jnp.stack(column_inverse((stacked[0], stacked[1]), groups, fields_count))

    def to_frequency(stacked):
        batch_len = stacked.shape[1]
        block_width = stacked.shape[3]
        shaped = stacked.reshape(
            2, batch_len, rows_count, fields_count, local_rows, 1, 1, block_width
        )
        arrived = lax.all_to_all(
            lax.all_to_all(shaped, "rows", split_axis=2, concat_axis=5, tiled=True),
            "fields",
            split_axis=3,
            concat_axis=6,
            tiled=True,
        )
        result = forward_columns(arrived.reshape(2, batch_len, local_rows, groups * block_width))
        return result

    def to_space(stacked):
        batch_len = stacked.shape[1]
        block_width = stacked.shape[3] // groups
        shaped = stacked.reshape(
            2, batch_len, 1, 1, local_rows, rows_count, fields_count, block_width
        )
        arrived = lax.all_to_all(
            lax.all_to_all(shaped, "rows", split_axis=5, concat_axis=2, tiled=True),
            "fields",
            split_axis=6,
            concat_axis=3,
            tiled=True,
        )
        result = inverse_rows(arrived.reshape(2, batch_len, total_rows, block_width))
        return result

    slab_spectra = jnp.stack(
        row_transform(
            (lax.all_to_all(sky_maps, "rows", split_axis=2, concat_axis=1, tiled=True), None), -1.0
        )
    )
    sky_spectra = to_frequency(slab_spectra)
    row_ids = lax.axis_index(("rows", "fields")) * local_rows + jnp.arange(
        local_rows, dtype=jnp.int32
    )
    freq_rows = jnp.where(row_ids < total_rows // 2, row_ids, row_ids - total_rows)[:, None]
    column_ids = jnp.arange(NC, dtype=jnp.int32)
    freq_cols = jnp.where(column_ids < NC // 2, column_ids, column_ids - NC)[None, :]
    scaled_rows = row_ratio * freq_rows
    radius_sq = freq_cols * freq_cols + scaled_rows * scaled_rows

    def band_mask(lower_cut, upper_cut):
        inside = (radius_sq >= lower_cut * lower_cut) & (radius_sq <= upper_cut * upper_cut)
        return inside.astype(jnp.float32)

    mask_temp = band_mask(band_cuts[0], band_cuts[1])
    mask_pol = band_mask(band_cuts[2], band_cuts[3])
    mask_out = band_mask(band_cuts[4], band_cuts[5])
    radius_floor = jnp.maximum(radius_sq, 1).astype(jnp.float32)
    cos_two = (freq_cols * freq_cols - scaled_rows * scaled_rows).astype(jnp.float32) / radius_floor
    sin_two = (2 * freq_cols * scaled_rows).astype(jnp.float32) / radius_floor
    along_x = (2 * freq_cols).astype(jnp.float32) / NC
    along_y = (2 * freq_rows).astype(jnp.float32) / total_rows
    raising = (-along_y + 0.0 * along_x, along_x + 0.0 * along_y)
    lowering = (along_y + 0.0 * along_x, along_x + 0.0 * along_y)
    rotation = (cos_two, sin_two)
    temp_modes = (sky_spectra[0, 0], sky_spectra[1, 0])
    stokes_q = (sky_spectra[0, 1], sky_spectra[1, 1])
    stokes_u = (sky_spectra[0, 2], sky_spectra[1, 2])
    e_modes = (
        -(cos_two * stokes_q[0] + sin_two * stokes_u[0]),
        -(cos_two * stokes_q[1] + sin_two * stokes_u[1]),
    )
    b_modes = (
        sin_two * stokes_q[0] - cos_two * stokes_u[0],
        sin_two * stokes_q[1] - cos_two * stokes_u[1],
    )
    temp_weight = mask_temp * filters[0]
    e_weight = mask_pol * filters[1]
    b_weight = mask_pol * filters[2]
    temp_bar = (temp_weight * temp_modes[0], temp_weight * temp_modes[1])
    e_bar = (e_weight * e_modes[0], e_weight * e_modes[1])
    b_bar = (b_weight * b_modes[0], b_weight * b_modes[1])
    grad_temp = complex_mul(raising, (wiener[0] * temp_bar[0], wiener[0] * temp_bar[1]))
    pol_sum = complex_mul((e_bar[0] - b_bar[1], e_bar[1] + b_bar[0]), rotation)
    pol_bar = (-pol_sum[0], -pol_sum[1])
    pol_rot = complex_mul((wiener[1] * e_bar[0], wiener[1] * e_bar[1]), rotation)
    pol_wiener = (-pol_rot[0], -pol_rot[1])
    spin_three = complex_mul(raising, pol_wiener)
    spin_one = complex_mul(lowering, pol_wiener)
    leg_spectra = jnp.stack(
        [
            jnp.stack([temp_bar[0], grad_temp[0], pol_bar[0], spin_three[0], spin_one[0]]),
            jnp.stack([temp_bar[1], grad_temp[1], pol_bar[1], spin_three[1], spin_one[1]]),
        ]
    )
    leg_maps = to_space(inverse_columns(leg_spectra))
    temp_leg = (leg_maps[0, 0], leg_maps[1, 0])
    grad_leg = (leg_maps[0, 1], leg_maps[1, 1])
    pol_leg = (leg_maps[0, 2], leg_maps[1, 2])
    three_leg = (leg_maps[0, 3], leg_maps[1, 3])
    one_leg = (leg_maps[0, 4], leg_maps[1, 4])
    temp_term = complex_mul(temp_leg, grad_leg)
    raise_term = conj_mul(pol_leg, three_leg)
    lower_term = conj_mul(one_leg, pol_leg)
    current = (
        temp_term[0] + 0.5 * (raise_term[0] + lower_term[0]),
        temp_term[1] + 0.5 * (raise_term[1] + lower_term[1]),
    )
    current_rows = jnp.stack(row_transform((current[0][None], current[1][None]), -1.0))
    current_modes = to_frequency(current_rows)
    out_weight = mask_out * response
    estimate_modes = complex_mul(
        lowering, (out_weight * current_modes[0, 0], out_weight * current_modes[1, 0])
    )
    estimate_stack = jnp.stack([estimate_modes[0][None], estimate_modes[1][None]])
    estimate_maps = to_space(inverse_columns(estimate_stack))
    slab_result = estimate_maps[:, 0]
    return lax.all_to_all(slab_result, "rows", split_axis=1, concat_axis=2, tiled=True)


SIDE = 128
TILE = (8, 128)
LEG_GROUPS = ((0, 2), (2, 2), (4, 1))
MESH = pl.DeviceIdType.MESH


def add_pair(a, b):
    imag = a[1] if b[1] is None else b[1] if a[1] is None else a[1] + b[1]
    return (a[0] + b[0], imag)


def sub_pair(a, b):
    imag = a[1] if b[1] is None else -b[1] if a[1] is None else a[1] - b[1]
    return (a[0] - b[0], imag)


def turn_pair(value, step, length, direction):
    real, imag = value
    if step == 0:
        return value
    if 4 * step == length:
        if imag is None:
            return (jnp.zeros_like(real), real if direction > 0 else -real)
        return (-imag, real) if direction > 0 else (imag, -real)
    angle = 2.0 * math.pi * step / length
    c, s = math.cos(angle), direction * math.sin(angle)
    if imag is None:
        return (real * c, real * s)
    if 8 * step == length:
        if direction > 0:
            return ((real - imag) * c, (real + imag) * c)
        return ((real + imag) * c, (imag - real) * c)
    if 8 * step == 3 * length:
        if direction > 0:
            return ((real + imag) * c, (imag - real) * c)
        return ((real - imag) * c, (real + imag) * c)
    return (real * c - imag * s, real * s + imag * c)


def short_transform(values, direction):
    length = len(values)
    if length == 1:
        return values
    even = short_transform(values[0::2], direction)
    odd = short_transform(values[1::2], direction)
    low, high = [], []
    for step in range(length // 2):
        turned = turn_pair(odd[step], step, length, direction)
        low.append(add_pair(even[step], turned))
        high.append(sub_pair(even[step], turned))
    return low + high


def split_number(x):
    top = x.astype(jnp.bfloat16)
    return top, (x - top.astype(jnp.float32)).astype(jnp.bfloat16)


def dot32(a, b):
    return jnp.dot(a, b, preferred_element_type=jnp.float32)


def matrix_left(table_ref, which, x):
    top, rest = split_number(x)
    m_top, m_rest = table_ref[which, 0], table_ref[which, 1]
    return dot32(m_top, top) + (dot32(m_top, rest) + dot32(m_rest, top))


def matrix_right(table_ref, which, x):
    top, rest = split_number(x)
    m_top, m_rest = table_ref[which, 0], table_ref[which, 1]
    return dot32(top, m_top) + (dot32(top, m_rest) + dot32(rest, m_top))


def lens_kernel(
    rows_count, fields_count, local_rows,
    cuts_ref, sky_hbm, filters_hbm, wiener_hbm, response_hbm, table_ref, twiddle_ref, out_ref,
    sky_ref, raw, weight_ref, slab_out, slab_in, spec_out, spec_in, weights, legs_out, legs_in, maps, current,
    cur_out, cur_in, est_out, est_in, fin_out, fin_in,
    slab_sem, spec_sem, legs_sem, cur_sem, est_sem, fin_sem, self_sem, load_sem,
):
    groups = rows_count * fields_count
    total_rows = groups * local_rows
    in_rows = total_rows // rows_count
    row_ratio = NC // total_rows
    my_r, my_f = lax.axis_index("rows"), lax.axis_index("fields")
    me = my_r * fields_count + my_f
    my_block = my_f * rows_count + my_r

    half = fields_count // 2
    my_half, my_spot = my_f // half, my_f % half

    def wrapped(value, length):
        return jnp.where(value >= length, value - length, value)

    row_at = [wrapped(my_r + d, rows_count) for d in range(rows_count)]
    spot_at = [wrapped(my_spot + d, half) for d in range(half)]
    side_at = [my_half * half, (1 - my_half) * half]

    def partner(q, sign):
        side = 1 - q // (rows_count * half)
        spot = sign * (q // rows_count + 1) % half
        return row_at[sign * (q + 1) % rows_count], side_at[side] + spot_at[spot]

    def peer_of(q):
        r, f = partner(q, 1)
        return r * fields_count + f

    def source_of(q):
        r, f = partner(q, -1)
        return r * fields_count + f

    def peer_block(q):
        r, f = partner(q, 1)
        return f * rows_count + r

    def source_block(q):
        r, f = partner(q, -1)
        return f * rows_count + r

    def target(q):
        r, f = partner(q, 1)
        return {"rows": r, "fields": f}

    def send(q, src, dst, sems):
        return pltpu.make_async_remote_copy(
            src_ref=src, dst_ref=dst, send_sem=sems[0], recv_sem=sems[1],
            device_id=target(q), device_id_type=MESH,
        )

    def send_row(q, src, dst, sems):
        return pltpu.make_async_remote_copy(
            src_ref=src, dst_ref=dst, send_sem=sems[0], recv_sem=sems[1],
            device_id={"rows": row_at[q]}, device_id_type=MESH,
        )

    def each_peer(body):
        for q in range(groups - 1):
            body(q)

    def each_row_peer(body):
        for q in range(1, rows_count):
            body(q)

    loads = [
        pltpu.make_async_copy(src, dst, load_sem.at[n])
        for n, (src, dst) in enumerate((
            (sky_hbm, sky_ref),
            (filters_hbm, raw.at[0:3]),
            (wiener_hbm, raw.at[3:5]),
            (response_hbm, raw.at[5]),
        ))
    ]
    for load in loads:
        load.start()

    barrier = pltpu.get_barrier_semaphore()

    def greet(q):
        pl.semaphore_signal(
            barrier, inc=1, device_id=target(q), device_id_type=MESH
        )

    each_peer(greet)
    loads[0].wait()
    tiles = sky_ref.shape[2] // SIDE
    for field in range(3):
        for t in range(tiles):
            slab_out[t // 8, field, :, t % 8, :] = sky_ref[field, :, t * SIDE:(t + 1) * SIDE]
    pl.semaphore_wait(barrier, groups - 1)

    def slab_copy(field, q, src_row):
        return send_row(
            q, slab_out.at[row_at[q], field], slab_in.at[src_row, field],
            (slab_sem.at[0, field, q], slab_sem.at[1, field, q]),
        )

    def own_slab(field):
        return pltpu.make_async_copy(
            slab_out.at[my_r, field], slab_in.at[my_r, field], self_sem.at[field]
        )

    for field in range(3):
        each_row_peer(lambda q: slab_copy(field, q, my_r).start())
        own_slab(field).start()

    low_index = lax.broadcasted_iota(jnp.int32, (SIDE, SIDE), 0)
    high_index = lax.broadcasted_iota(jnp.int32, (SIDE, SIDE), 1)
    column_ids = low_index + SIDE * high_index
    freq_cols = jnp.where(column_ids < NC // 2, column_ids, column_ids - NC)

    def row_frequency(row):
        row_id = me * local_rows + row
        return jnp.where(row_id < total_rows // 2, row_id, row_id - total_rows)

    def weigh(row, carry):
        scaled = row_ratio * row_frequency(row)
        radius_sq = freq_cols * freq_cols + scaled * scaled

        def mask(n):
            low, high = cuts_ref[2 * n], cuts_ref[2 * n + 1]
            inside = (radius_sq >= low * low) & (radius_sq <= high * high)
            return inside.astype(jnp.float32)

        pol = mask(1)
        weights[0, row] = mask(0) * weight_ref[0, row].T
        weights[1, row] = pol * weight_ref[1, row].T
        weights[2, row] = pol * weight_ref[2, row].T
        weights[3, row] = weight_ref[3, row].T
        weights[4, row] = weight_ref[4, row].T
        weights[5, row] = mask(2) * weight_ref[5, row].T
        return carry


    def spec_copy(field, row, q, src_block):
        return send(
            q, spec_out.at[field, row, peer_of(q)], spec_in.at[field, row, :, src_block],
            (spec_sem.at[0, field, row, q], spec_sem.at[1, field, row, q]),
        )

    def own_spec(field, row):
        return pltpu.make_async_copy(
            spec_out.at[field, row, me], spec_in.at[field, row, :, my_block],
            self_sem.at[3 + field * local_rows + row],
        )

    def spec_start(field, row):
        each_peer(lambda q: spec_copy(field, row, q, my_block).start())
        own_spec(field, row).start()

    def row_step(field, carry):
        each_row_peer(
            lambda q: slab_copy(field, q, row_at[rows_count - q]).wait_recv()
        )
        own_slab(field).wait()
        values = [
            (slab_in[y // in_rows, field, y % in_rows], None) for y in range(total_rows)
        ]
        for k, (real, imag) in enumerate(short_transform(values, -1)):
            spec_out[field, k % local_rows, k // local_rows, 0] = real
            spec_out[field, k % local_rows, k // local_rows, 1] = (
                jnp.zeros_like(real) if imag is None else imag
            )
        spec_start(field, 0)
        return carry

    lax.fori_loop(0, 3, row_step, 0)

    def later_rows(n, carry):
        spec_start(n % 3, 1 + n // 3)
        return carry

    lax.fori_loop(0, 3 * (local_rows - 1), later_rows, 0)

    def spec_wait(row):
        def step(field, carry):
            each_peer(lambda q: spec_copy(field, row, q, source_block(q)).wait_recv())
            own_spec(field, row).wait()
            return carry

        lax.fori_loop(0, 3, step, 0)

    cos_f, sin_f, cos_b, sin_b = 0, 1, 2, 3

    def side_by_side(pieces, axis):
        return pieces[0] if len(pieces) == 1 else jnp.concatenate(pieces, axis=axis)

    def long_forward(pieces):
        y = matrix_left(table_ref, 0, side_by_side(pieces, 1))
        c, s = twiddle_ref[cos_f], twiddle_ref[sin_f]
        turned = []
        for n in range(len(pieces)):
            yr, yi = y[:SIDE, n * SIDE:(n + 1) * SIDE], y[SIDE:, n * SIDE:(n + 1) * SIDE]
            turned.append(jnp.concatenate([yr * c - yi * s, yr * s + yi * c], axis=1))
        z = matrix_right(table_ref, 1, side_by_side(turned, 0))
        return [
            (z[n * SIDE:(n + 1) * SIDE, :SIDE], z[n * SIDE:(n + 1) * SIDE, SIDE:])
            for n in range(len(pieces))
        ]

    def long_inverse(pairs):
        stacks = [jnp.concatenate([pair[0], pair[1]], axis=1) for pair in pairs]
        u = matrix_right(table_ref, 0, side_by_side(stacks, 0))
        c, s = twiddle_ref[cos_b], twiddle_ref[sin_b]
        turned = []
        for n in range(len(pairs)):
            ur, ui = u[n * SIDE:(n + 1) * SIDE, :SIDE], u[n * SIDE:(n + 1) * SIDE, SIDE:]
            turned.append(jnp.concatenate([ur * c - ui * s, ur * s + ui * c], axis=0))
        x = matrix_left(table_ref, 1, side_by_side(turned, 1))
        return [
            x[:, n * SIDE:(n + 1) * SIDE].reshape((2, groups) + TILE)
            for n in range(len(pairs))
        ]

    leg_self = 3 + 3 * local_rows

    def legs_copy(row, g, q, src_index):
        first, count = LEG_GROUPS[g]
        return send(
            q, legs_out.at[row, first:first + count, :, peer_block(q)],
            legs_in.at[row, src_index, first:first + count],
            (legs_sem.at[0, row, g, q], legs_sem.at[1, row, g, q]),
        )

    def own_legs(row, g):
        first, count = LEG_GROUPS[g]
        return pltpu.make_async_copy(
            legs_out.at[row, first:first + count, :, my_block],
            legs_in.at[row, me, first:first + count],
            self_sem.at[leg_self + row * len(LEG_GROUPS) + g],
        )

    def slopes(row):
        along_x = (2 * freq_cols).astype(jnp.float32) / NC
        along_y = (2 * row_frequency(row)).astype(jnp.float32) / total_rows
        return along_x, along_y

    def leg_step(row, carry):
        spec_wait(row)
        temp, stokes_q, stokes_u = long_forward(
            [spec_in[field, row].reshape(2 * SIDE, SIDE) for field in range(3)]
        )
        scaled = row_ratio * row_frequency(row)
        radius_sq = freq_cols * freq_cols + scaled * scaled
        floor = jnp.maximum(radius_sq, 1).astype(jnp.float32)
        cos2 = (freq_cols * freq_cols - scaled * scaled).astype(jnp.float32) / floor
        sin2 = (2 * freq_cols * scaled).astype(jnp.float32) / floor
        along_x, along_y = slopes(row)
        raising, lowering = (-along_y, along_x), (along_y, along_x)
        rot = (cos2, sin2)
        w_t, w_e, w_b = weights[0, row], weights[1, row], weights[2, row]
        w_gt, w_ge = weights[3, row], weights[4, row]
        t_bar = (w_t * temp[0], w_t * temp[1])
        e_bar = tuple(-w_e * (cos2 * a + sin2 * b) for a, b in zip(stokes_q, stokes_u))
        b_bar = tuple(w_b * (sin2 * a - cos2 * b) for a, b in zip(stokes_q, stokes_u))
        g = complex_mul((w_gt * t_bar[0], w_gt * t_bar[1]), raising)
        p = complex_mul((b_bar[1] - e_bar[0], -(e_bar[1] + b_bar[0])), rot)
        w = complex_mul((-w_ge * e_bar[0], -w_ge * e_bar[1]), rot)
        h3 = complex_mul(w, raising)
        h1 = complex_mul(w, lowering)
        legs = (t_bar, g, p, h3, h1)
        for n, (first, count) in enumerate(LEG_GROUPS):
            for k, leg_map in enumerate(long_inverse(legs[first:first + count])):
                legs_out[row, first + k] = leg_map
            each_peer(lambda q: legs_copy(row, n, q, me).start())
            own_legs(row, n).start()
        return carry

    for load in loads[1:]:
        load.wait()

    def spread(n, carry):
        for j in range(8):
            start = pl.multiple_of((n * 8 + j) * SIDE, SIDE)
            weight_ref[:, :, n * 8 + j, :] = raw[:, :, pl.ds(start, SIDE)]
        return carry

    lax.fori_loop(0, SIDE // 8, spread, 0)
    lax.fori_loop(0, local_rows, weigh, 0)
    lax.fori_loop(0, local_rows, leg_step, 0)

    for field in range(3):
        each_row_peer(lambda q: slab_copy(field, q, my_r).wait_send())

    def spec_left(n, carry):
        each_peer(lambda q: spec_copy(n % 3, n // 3, q, my_block).wait_send())
        return carry

    lax.fori_loop(0, 3 * local_rows, spec_left, 0)

    def leg_wait(g):
        def step(row, carry):
            each_peer(lambda q: legs_copy(row, g, q, source_of(q)).wait_recv())
            own_legs(row, g).wait()
            return carry

        lax.fori_loop(0, local_rows, step, 0)

    def map_step(n, carry):
        values = [
            (legs_in[k % local_rows, k // local_rows, n, 0],
             legs_in[k % local_rows, k // local_rows, n, 1])
            for k in range(total_rows)
        ]
        for y, (real, imag) in enumerate(short_transform(values, 1)):
            maps[n, 0, y] = real
            maps[n, 1, y] = imag
        return carry

    for g, (first, count) in enumerate(LEG_GROUPS):
        leg_wait(g)
        lax.fori_loop(first, first + count, map_step, 0)

    def product_step(y, carry):
        a, g, p, h3, h1 = [(maps[n, 0, y], maps[n, 1, y]) for n in range(5)]
        ag, ph, hp = complex_mul(a, g), conj_mul(p, h3), conj_mul(h1, p)
        current[0, y] = ag[0] + 0.5 * (ph[0] + hp[0])
        current[1, y] = ag[1] + 0.5 * (ph[1] + hp[1])
        return carry

    lax.fori_loop(0, total_rows, product_step, 0)

    values = [(current[0, y], current[1, y]) for y in range(total_rows)]
    for k, (real, imag) in enumerate(short_transform(values, -1)):
        cur_out[k % local_rows, k // local_rows, 0] = real
        cur_out[k % local_rows, k // local_rows, 1] = imag
    cur_self = leg_self + len(LEG_GROUPS) * local_rows
    est_self = cur_self + local_rows

    def cur_copy(row, q, src_block):
        return send(
            q, cur_out.at[row, peer_of(q)], cur_in.at[row, :, src_block],
            (cur_sem.at[0, row, q], cur_sem.at[1, row, q]),
        )

    def own_cur(row):
        return pltpu.make_async_copy(
            cur_out.at[row, me], cur_in.at[row, :, my_block], self_sem.at[cur_self + row]
        )

    def cur_start(row, carry):
        each_peer(lambda q: cur_copy(row, q, my_block).start())
        own_cur(row).start()
        return carry

    lax.fori_loop(0, local_rows, cur_start, 0)

    def legs_left(row, carry):
        for g in range(len(LEG_GROUPS)):
            each_peer(lambda q: legs_copy(row, g, q, me).wait_send())
        return carry

    lax.fori_loop(0, local_rows, legs_left, 0)

    def est_copy(row, q, src_index):
        return send(
            q, est_out.at[row, :, peer_block(q)], est_in.at[row, src_index],
            (est_sem.at[0, row, q], est_sem.at[1, row, q]),
        )

    def own_est(row):
        return pltpu.make_async_copy(
            est_out.at[row, :, my_block], est_in.at[row, me], self_sem.at[est_self + row]
        )

    def estimate_step(row, carry):
        each_peer(lambda q: cur_copy(row, q, source_block(q)).wait_recv())
        own_cur(row).wait()
        (modes,) = long_forward([cur_in[row].reshape(2 * SIDE, SIDE)])
        along_x, along_y = slopes(row)
        w = weights[5, row]
        estimate = complex_mul((w * modes[0], w * modes[1]), (along_y, along_x))
        (est_out[row],) = long_inverse([estimate])
        each_peer(lambda q: est_copy(row, q, me).start())
        own_est(row).start()
        return carry

    lax.fori_loop(0, local_rows, estimate_step, 0)

    def cur_left(row, carry):
        each_peer(lambda q: cur_copy(row, q, my_block).wait_send())
        return carry

    lax.fori_loop(0, local_rows, cur_left, 0)

    def est_wait(row, carry):
        each_peer(lambda q: est_copy(row, q, source_of(q)).wait_recv())
        own_est(row).wait()
        return carry

    lax.fori_loop(0, local_rows, est_wait, 0)

    values = [
        (est_in[k % local_rows, k // local_rows, 0], est_in[k % local_rows, k // local_rows, 1])
        for k in range(total_rows)
    ]
    for y, (real, imag) in enumerate(short_transform(values, 1)):
        fin_out[y // in_rows, 0, y % in_rows] = real
        fin_out[y // in_rows, 1, y % in_rows] = imag

    def fin_copy(q, src_row):
        return send_row(
            q, fin_out.at[row_at[q]], fin_in.at[src_row],
            (fin_sem.at[0, q], fin_sem.at[1, q]),
        )

    each_row_peer(lambda q: fin_copy(q, my_r).start())
    own_fin = pltpu.make_async_copy(
        fin_out.at[my_r], fin_in.at[my_r], self_sem.at[est_self + local_rows]
    )
    own_fin.start()

    def est_left(row, carry):
        each_peer(lambda q: est_copy(row, q, me).wait_send())
        return carry

    lax.fori_loop(0, local_rows, est_left, 0)
    each_row_peer(lambda q: fin_copy(q, row_at[rows_count - q]).wait_recv())
    own_fin.wait()
    for part in range(2):
        for t in range(tiles):
            out_ref[part, :, t * SIDE:(t + 1) * SIDE] = fin_in[t // 8, part, :, t % 8, :]

    each_row_peer(lambda q: fin_copy(q, my_r).wait_send())


def long_tables(total_rows):
    index = np.arange(SIDE)
    angle = 2.0 * np.pi * (index[:, None] * index[None, :] % SIDE) / SIDE
    c, s = np.cos(angle), np.sin(angle)
    forward = np.block([[c, s], [-s, c]]).astype(np.float32)
    tables = np.stack([forward, forward.T])
    top = tables.astype(jnp.bfloat16)
    rest = (tables - top.astype(np.float32)).astype(jnp.bfloat16)
    turn = 2.0 * np.pi * (index[:, None] * index[None, :]) / NC
    scale = 1.0 / (NC * total_rows)
    twiddle = np.stack(
        [np.cos(turn), -np.sin(turn), scale * np.cos(turn), scale * np.sin(turn)]
    ).astype(np.float32)
    return np.stack([top, rest], axis=1), twiddle


def fused_body(rows_count, fields_count, sky_maps, band_cuts, filters, wiener, response):
    groups = rows_count * fields_count
    local_rows = response.shape[0]
    total_rows = local_rows * groups
    in_rows = total_rows // rows_count
    table, twiddle = long_tables(total_rows)
    vmem = pl.BlockSpec(memory_space=pltpu.VMEM)
    f32 = jnp.float32
    dma = pltpu.SemaphoreType.DMA
    slab = pltpu.VMEM((rows_count, 3, in_rows) + TILE, f32)
    chunk = pltpu.VMEM((local_rows, groups, 2) + TILE, f32)
    lines = pltpu.VMEM((local_rows, 2, groups) + TILE, f32)
    final = pltpu.VMEM((rows_count, 2, in_rows) + TILE, f32)
    return pl.pallas_call(
        functools.partial(lens_kernel, rows_count, fields_count, local_rows),
        out_shape=jax.ShapeDtypeStruct((2,) + sky_maps.shape[1:], f32),
        in_specs=[pl.BlockSpec(memory_space=pltpu.SMEM)]
        + [pl.BlockSpec(memory_space=pl.ANY)] * 4
        + [vmem] * 2,
        out_specs=vmem,
        scratch_shapes=[
            pltpu.VMEM(sky_maps.shape, f32),
            pltpu.VMEM((6, local_rows, NC), f32),
            pltpu.VMEM((6, local_rows, SIDE, SIDE), f32),
            slab, slab,
            pltpu.VMEM((3, local_rows, groups, 2) + TILE, f32),
            pltpu.VMEM((3, local_rows, 2, groups) + TILE, f32),
            pltpu.VMEM((6, local_rows, SIDE, SIDE), f32),
            pltpu.VMEM((local_rows, 5, 2, groups) + TILE, f32),
            pltpu.VMEM((local_rows, groups, 5, 2) + TILE, f32),
            pltpu.VMEM((5, 2, total_rows) + TILE, f32),
            pltpu.VMEM((2, total_rows) + TILE, f32),
            chunk, lines, lines, chunk, final, final,
            dma((2, 3, rows_count)), dma((2, 3, local_rows, groups - 1)),
            dma((2, local_rows, len(LEG_GROUPS), groups - 1)),
            dma((2, local_rows, groups - 1)), dma((2, local_rows, groups - 1)),
            dma((2, rows_count)), dma((4 + (5 + len(LEG_GROUPS)) * local_rows,)),
            dma((4,)),
        ],
        compiler_params=pltpu.CompilerParams(
            collective_id=0, has_side_effects=True, vmem_limit_bytes=60 * 1024 * 1024
        ),
        name="lens",
    )(band_cuts, sky_maps, filters, wiener, response, jnp.asarray(table), jnp.asarray(twiddle))


def solution(mesh):
    placed = (
        P("sims", "rows", "fields"),
        P(),
        P(None, ("rows", "fields"), None),
        P(None, ("rows", "fields"), None),
        P(("rows", "fields"), None),
    )
    rows_count, fields_count = mesh.shape["rows"], mesh.shape["fields"]
    groups = rows_count * fields_count

    def choose(sky_maps, *rest):
        fits = (
            NC == SIDE * SIDE
            and fields_count % 2 == 0
            and NC // groups == TILE[0] * TILE[1]
            and sky_maps.shape[1] % 8 == 0
            and sky_maps.shape[1] * rows_count in (16, 32, 64)
        )
        if fits:
            return fused_body(rows_count, fields_count, sky_maps, *rest)
        return body(sky_maps, *rest)

    return jax.shard_map(
        choose, mesh=mesh, in_specs=placed, out_specs=P("sims", "rows", "fields"), check_vma=False
    )
```
